128 devices in a mesh: img: 32 (over y, z, core), grp: 4 (over x).
Axes of the slice: x: 4, y: 4, z: 4, core: 2. Of those that a mesh axis runs over, the one named last changes fastest.
Arguments:
- images: bfloat16 [49152, 9216], P(('img', 'grp')), may hold values from -64 to 64, as said below
- expansion_basis: bfloat16 [9216, 960], P(None, 'img'), may hold values from -0.0625 to 0.0625
- block_sizes: int32 [16], replicated, may hold values from 1 to 80, 480 in all
- keep_count: int32 [16], replicated, may hold values from 1 to 8
- start_block: float32 [16, 80, 8], replicated, may hold values from -6 to 6
Outputs:
- features: float32 [49152, 256], P(('img', 'grp'))
- values: float32 [16, 8], replicated
The draws below stay inside these ranges and needn't reach their ends.
Inputs may be any that keep to these rules, and one draw needn't show every extreme that they name: `images`: pixel values of order one. `block_sizes`: the 16 sizes sum to 480.
All inputs are finite; a program needn't handle non-finite values.
Results may differ from the reference program's by a relative error of at most 0.025.
Values may be sent and summed in bfloat16 or wider, within the bound.
A program may use at most 128 MiB of HBM per device.

```python
import math
import jax
import jax.numpy as jnp
import numpy as np
from jax import lax

PIX = 9216
NMAX = 80
L = 16
S = 480
KMAX = 8
ITERS = 3
P_SIZE = 384
NPART = 49152


def draw_images(key, part):
    first = jax.random.fold_in(key, 11)
    second = jax.random.fold_in(key, 23)
    third = jax.random.fold_in(key, 37)
    order = jnp.arange(NPART, dtype=jnp.float32) / max(NPART - 1, 1)
    row_scale = jnp.exp(jnp.log(3.0) * order) * jax.random.uniform(first, (NPART,), jnp.float32, 0.7, 1.4)
    column_scale = jnp.exp(jax.random.uniform(second, (PIX,), jnp.float32, jnp.log(0.3), jnp.log(3.0)))
    noise = jnp.clip(jax.random.normal(third, (NPART, PIX), jnp.float32), -5.0, 5.0)
    return (noise * row_scale[:, None] * column_scale[None, :]).astype(jnp.bfloat16)


def place_ends(values, key, low, top_value):
    extent = values.shape
    place = [jax.random.randint(jax.random.fold_in(key, axis), (), 0, extent[axis]) for axis in range(len(extent))]
    values = values.at[tuple(place)].set(low)
    longest = extent.index(max(extent))
    place[longest] = (place[longest] + 1) % extent[longest]
    return values.at[tuple(place)].set(top_value)


def level_of(key, dims, shards, low, high):
    def one(position, parts):
        heights = jax.random.uniform(jax.random.fold_in(jax.random.fold_in(key, 6), position), (parts,), jnp.float32, low / len(shards), high / len(shards))
        return jnp.repeat(jnp.exp(heights), dims[position] // parts).reshape((-1,) + (1,) * (len(dims) - position - 1))

    gain = one(*shards[0])
    for cut in shards[1:]:
        gain = gain * one(*cut)
    return gain


def split_up(count, total, most, skew):
    loads = [(1 << 20) // math.isqrt(grade ** skew) + 1 for grade in range(2, count + 1)]
    surplus, given = total - most - (count - 1), [1] * (count - 1)
    while surplus > 0:
        movable = [i for i in range(count - 1) if given[i] < most]
        whole, budget = sum([loads[i] for i in movable]), surplus
        for i in movable:
            addition = min(most - given[i], max(1, budget * loads[i] // whole), surplus)
            given[i] = given[i] + addition
            surplus = surplus - addition
    return np.array([most] + given)


def ragged(rng, number_of, total, bound, slope):
    if number_of == 2:
        one = jax.random.randint(rng, (), max(1, total - bound), min(bound, total - 1) + 1)
        return jnp.stack([one, total - one])
    lengths = jnp.asarray(split_up(number_of, total, bound, slope), jnp.int32)
    pairs = (number_of - 1) // 2
    donor, sink = lengths[1:1 + 2 * pairs:2], lengths[2:2 + 2 * pairs:2]
    margin = jnp.minimum(donor - 1, bound - sink)
    moved = jax.random.randint(jax.random.fold_in(rng, 1), (pairs,), 0, 1 << 20) % (margin + 1)
    lengths = lengths.at[1:1 + 2 * pairs:2].set(donor - moved).at[2:2 + 2 * pairs:2].set(sink + moved)
    return lengths[jax.random.permutation(jax.random.fold_in(rng, 2), number_of)]


def bell_draw(rng, dims, spread, bound, pieces=(), held_as=jnp.bfloat16):
    drawn = spread * jax.random.normal(rng, dims, jnp.float32)
    if pieces:
        drawn = drawn * level_of(rng, dims, pieces, -0.22, 0.18)
    return jnp.clip(drawn, -bound, bound).astype(held_as)


def setup_inputs(seed: int = 0) -> dict:
    key_list = jax.random.split(jax.random.key(seed), 6)
    images = draw_images(jax.random.fold_in(key_list[5], 71), 0)
    expansion_basis = bell_draw(key_list[1], (PIX, 2 * S), PIX ** -0.5, 0.0625, ((1, 32),))
    block_sizes = ragged(key_list[2], L, S, NMAX, 2).astype(jnp.int32)
    keep_count = place_ends(jax.random.randint(key_list[3], (L,), 1, KMAX + 1), jax.random.fold_in(key_list[3], 1), 1, KMAX).astype(jnp.int32)
    start_block = bell_draw(key_list[4], (L, NMAX, KMAX), 1.0, 6.0, (), jnp.float32)
    return dict(images=images, expansion_basis=expansion_basis, block_sizes=block_sizes, keep_count=keep_count, start_block=start_block)


HIGH = lax.Precision.HIGHEST

def selector(block_sizes, total, count, width):
    offsets = jnp.cumsum(block_sizes) - block_sizes
    column = jnp.arange(total, dtype=jnp.int32)[:, None, None]
    inside = jnp.arange(width, dtype=jnp.int32)[None, None, :]
    hit = (column == offsets[None, :, None] + inside) & (inside < block_sizes[None, :, None])
    return hit.astype(jnp.bfloat16).reshape(total, count * width)

def subspace(cover, block_sizes, keep_count, start_block):
    width = cover.shape[1]
    ranks = start_block.shape[2]
    inside = jnp.arange(width, dtype=jnp.int32)[None, :, None] < block_sizes[:, None, None]
    keep = jnp.minimum(keep_count, (block_sizes + 1) // 2)
    current = jnp.where(inside, start_block, jnp.zeros_like(start_block))
    for turn in range(ITERS):
        product = jnp.einsum('bij,bjk->bik', cover, current, precision=HIGH)
        columns = []
        for column_id in range(ranks):
            vector = product[:, :, column_id]
            for earlier in columns:
                vector = vector - lax.optimization_barrier(jnp.sum(earlier * vector, axis=1, keepdims=True)) * earlier
            length = jnp.sqrt(lax.optimization_barrier(jnp.sum(vector * vector, axis=1, keepdims=True)))
            alive = (column_id < keep)[:, None]
            columns.append(jnp.where(alive, vector / length, jnp.zeros_like(vector)))
        current = jnp.stack(columns, axis=2)
    product = jnp.einsum('bij,bjk->bik', cover, current, precision=HIGH)
    found = lax.optimization_barrier(jnp.sum(current * product, axis=1))
    return (current, found)

def reference(images, expansion_basis, block_sizes, keep_count, start_block):
    count_all = images.shape[0] // P_SIZE
    pick = selector(block_sizes, S, L, NMAX)
    scale = 1.0 / (2 * images.shape[0])

    def accumulate(total, span_rows):
        coeffs = jnp.dot(span_rows, expansion_basis, preferred_element_type=jnp.float32).astype(jnp.bfloat16)
        samples = coeffs.reshape(2 * P_SIZE, S)
        padded = jnp.dot(samples, pick, preferred_element_type=jnp.float32).astype(jnp.bfloat16)
        wide = padded.astype(jnp.float32).reshape(2 * P_SIZE, L, NMAX)
        partial_value = jnp.einsum('rli,rlj->lij', wide, wide, precision=HIGH) * scale
        return (total + partial_value, padded)
    start_total = jnp.zeros((L, NMAX, NMAX), jnp.float32)
    cover, padded_all = lax.scan(accumulate, start_total, images.reshape(count_all, P_SIZE, PIX))
    vectors, found = subspace(cover, block_sizes, keep_count, start_block)
    rounded = vectors.astype(jnp.bfloat16).astype(jnp.float32)
    wide_all = padded_all.reshape(count_all * 2 * P_SIZE, L, NMAX).astype(jnp.float32)
    features = jnp.einsum('rli,lij->rlj', wide_all, rounded, precision=HIGH)
    return (features.reshape(images.shape[0], 2 * L * KMAX), found)
```

```python
import functools
import heapq

import jax
import jax.numpy as jnp
from jax import lax
from jax.experimental import pallas as pl
from jax.experimental.pallas import tpu as pltpu
from jax.sharding import Mesh
from jax.sharding import PartitionSpec as P

NMAX = 80
L = 16
S = 480
KMAX = 8
ITERS = 3
AXES = ("img_0", "img_1", "img_2", "grp")
IMG = AXES[:3]
IMG_GRP = AXES
HIGH = lax.Precision.HIGHEST
MESH = pl.DeviceIdType.MESH

KC = 256
SUBS = 4
ROUNDS = 6
CHUNKS = 16 + (ROUNDS - 1) * SUBS
ROWS = 32
BLOCK = ROWS * KC * 2


class Plan:
    def __init__(self, ahead=2, rate=44e3, hop=1.9, d_rate=500e3, d_hop=1.1, dot=0.3):
        self.program = []
        self.sems = {}
        busy = {}
        now = 0.0
        heap = []
        arrived = {}
        ready = []

        def send(key, link, size):
            sem = self.sems.setdefault(key, len(self.sems))
            fast = link == "d"
            begin = max(busy.get(link, 0.0), now)
            end = begin + size / (d_rate if fast else rate)
            busy[link] = end
            heapq.heappush(heap, (end + (d_hop if fast else hop), sem, key))
            self.program.append(("send", key))

        def axes(sub):
            return ("y", "z") if sub < 2 else ("z", "y")

        def way(sub):
            return ("+", "-") if sub % 2 == 0 else ("-", "+")

        def start_round(r):
            for sub in range(SUBS):
                a = axes(sub)[0]
                send(("1", r, sub, 0), a + "+", BLOCK)
                send(("1", r, sub, 1), a + "-", BLOCK)

        def spread(kind, rest, axis, sub, size):
            send((kind, *rest, 0), axis + "+", size)
            send((kind, *rest, 1), axis + "-", size)

        def got(group, need):
            arrived[group] = arrived.get(group, 0) + 1
            return arrived[group] == need

        def half_done(chunk):
            send(("D", chunk), "d", 16 * BLOCK)
            if got(("C", chunk), 2):
                ready.append(chunk)

        started = 0
        while started < min(ahead, ROUNDS):
            start_round(started)
            started += 1
        while heap or ready:
            if ready and (not heap or heap[0][0] > now or len(ready) > 3):
                chunk = ready.pop(0)
                self.program.append(("dot", chunk))
                now += dot
                continue
            when, _, key = heapq.heappop(heap)
            now = max(now, when) + 0.02
            self.program.append(("wait", key))
            kind = key[0]
            if kind in ("1", "2"):
                _, r, sub, j = key
                axis = axes(sub)[0 if kind == "1" else 1]
                size = BLOCK if kind == "1" else 4 * BLOCK
                if j == sub % 2:
                    send((kind, r, sub, 2), axis + way(sub)[0], size)
                if kind == "1" and got(("1", r, sub), 3):
                    spread("2", (r, sub), axes(sub)[1], sub, 4 * BLOCK)
                    if r == 0:
                        spread("X", (sub, 0), "x", sub, 4 * BLOCK)
                    if sub == SUBS - 1 and started < ROUNDS:
                        start_round(started)
                        started += 1
                if kind == "2":
                    if r == 0:
                        spread("X", (sub, 1 + j), "x", sub, 4 * BLOCK)
                    if got(("2", r, sub), 3):
                        half_done(("own", sub) if r == 0 else ("all", r, sub))
            elif kind == "X":
                _, sub, piece, j = key
                if j == sub % 2:
                    send(("X", sub, piece, 2), "x" + way(sub)[0], 4 * BLOCK)
                if got(("X", sub, j), 4):
                    half_done(("far", j, sub))
            else:
                if got(("C", key[1]), 2):
                    ready.append(key[1])
        self.end = now


def gather_dot(plan, images, own, coeffs, held, pixels, total, fill_sem, send_sem, recv_sem):
    y, z, c, x = (lax.axis_index(a) for a in AXES)

    def turn(v, by):
        return lax.rem(v + (by + 4), 4)

    def device(axis, by):
        spot = {"y": y, "z": z, "x": x}
        spot[axis] = turn(spot[axis], by)
        return (spot["y"], spot["z"], c, spot["x"])

    sibling = (y, z, 1 - c, x)
    barrier = pltpu.get_barrier_semaphore()
    fills = [
        pltpu.make_async_copy(own.at[pl.ds(4 * x, 4)], held.at[pl.ds(4 * x, 4), y, z, c], fill_sem.at[0]),
        pltpu.make_async_copy(own.at[pl.ds(16, CHUNKS - 16)], held.at[pl.ds(16, CHUNKS - 16), y, z, c], fill_sem.at[1]),
        pltpu.make_async_copy(images, pixels, fill_sem.at[2]),
    ]
    for fill in fills:
        fill.start()
    for axis in "yzx":
        for by in (1, -1):
            pl.semaphore_signal(barrier, inc=1, device_id=device(axis, by), device_id_type=MESH)
    pl.semaphore_signal(barrier, inc=1, device_id=sibling, device_id_type=MESH)
    total[...] = jnp.zeros_like(total)
    pl.semaphore_wait(barrier, 7)
    fills[0].wait()
    fills[1].wait()

    SHIFT = (-1, 1, 2)

    def index(chunk):
        if chunk[0] == "own":
            return 4 * x + chunk[1]
        if chunk[0] == "far":
            return 4 * turn(x, SHIFT[chunk[1]]) + chunk[2]
        return 16 + (chunk[1] - 1) * SUBS + chunk[2]

    def copy_of(key):
        kind = key[0]
        if kind == "D":
            part = held.at[index(key[1]), :, :, c]
            where = sibling
        else:
            j = key[-1]
            sub = key[2] if kind != "X" else key[1]
            step = (1, -1)[j] if j < 2 else (1, -1)[sub % 2]
            back = 0 if j < 2 else -step
            first = sub < 2
            if kind == "1":
                k = index(("own", sub) if key[1] == 0 else ("all", key[1], sub))
                part = held.at[k, turn(y, back), z, c] if first else held.at[k, y, turn(z, back), c]
                where = device("y" if first else "z", step)
            elif kind == "2":
                k = index(("own", sub) if key[1] == 0 else ("all", key[1], sub))
                part = held.at[k, :, turn(z, back), c] if first else held.at[k, turn(y, back), :, c]
                where = device("z" if first else "y", step)
            else:
                k = 4 * turn(x, back) + sub
                shift = (0, *SHIFT)[key[2]]
                if key[2] == 3:
                    shift = 2
                part = held.at[k, :, turn(z, shift), c] if first else held.at[k, turn(y, shift), :, c]
                where = device("x", step)
        sem = plan.sems[key]
        return pltpu.make_async_remote_copy(
            src_ref=part, dst_ref=part, send_sem=send_sem, recv_sem=recv_sem.at[sem],
            device_id=where, device_id_type=MESH,
        )

    sent = []
    loaded = False
    for op, what in plan.program:
        if op == "send":
            copy = copy_of(what)
            copy.start()
            sent.append(copy)
        elif op == "wait":
            copy_of(what).wait_recv()
        else:
            if not loaded:
                fills[2].wait()
                loaded = True
            k = index(what)
            block = held[k].reshape(32 * ROWS, KC)
            rows = pixels[:, pl.ds(pl.multiple_of(k * KC, KC), KC)]
            total[...] += lax.dot_general(
                rows, block, (((1,), (1,)), ((), ())), preferred_element_type=jnp.float32
            )
    for copy in sent:
        copy.wait_send()
    coeffs[...] = total[...].astype(coeffs.dtype)


def gathered_coeffs(images, basis):
    plan = Plan()
    rows = images.shape[0]
    own = jnp.pad(basis.T, ((0, ROWS - basis.shape[1]), (0, 0)))
    own = own.reshape(ROWS, CHUNKS, KC).swapaxes(0, 1)
    any_ = pl.BlockSpec(memory_space=pl.ANY)
    return pl.pallas_call(
        functools.partial(gather_dot, plan),
        out_shape=jax.ShapeDtypeStruct((rows, 32 * ROWS), jnp.bfloat16),
        in_specs=[any_, any_],
        out_specs=pl.BlockSpec(memory_space=pltpu.VMEM),
        scratch_shapes=[
            pltpu.VMEM((CHUNKS, 4, 4, 2, ROWS, KC), jnp.bfloat16),
            pltpu.VMEM(images.shape, jnp.bfloat16),
            pltpu.VMEM((rows, 32 * ROWS), jnp.float32),
            pltpu.SemaphoreType.DMA((3,)),
            pltpu.SemaphoreType.DMA,
            pltpu.SemaphoreType.DMA((len(plan.sems),)),
        ],
        compiler_params=pltpu.CompilerParams(
            collective_id=0, has_side_effects=True, vmem_limit_bytes=48 * 1024 * 1024
        ),
    )(images, own)


def cut_along(shard, dim, peers):
    shape = shard.shape
    tiles = shard.reshape(*shape[:dim], peers, shape[dim] // peers, *shape[dim + 1 :])
    return jnp.moveaxis(tiles, dim, 0)


def sum_at_owner(shard, axis, dim):
    peers = lax.axis_size(axis)
    tiles = lax.all_to_all(cut_along(shard, dim, peers), axis, 0, 0, tiled=True)
    return jnp.sum(tiles, axis=0)


def summed_rows(shard, axes, dim):
    far, near = axes
    tiles = cut_along(shard, dim, lax.axis_size(far))
    nearer = sum_at_owner(tiles, near, dim + 1)
    arrived = lax.all_to_all(nearer, far, split_axis=0, concat_axis=0, tiled=True)
    return arrived.sum(axis=0)


def padded_to(lines, peers):
    spare = -len(lines) % peers
    return jnp.pad(lines, [(0, spare)] + [(0, 0)] * (lines.ndim - 1))


def sent_to_all(shard, axis):
    peers = lax.axis_size(axis)
    return lax.all_to_all(
        jnp.broadcast_to(shard[None], (peers, *shard.shape)), axis, 0, 0, tiled=True
    )


def in_order(tiles, dim):
    shape = list(tiles.shape[1:])
    shape[dim] *= tiles.shape[0]
    return jnp.moveaxis(tiles, 0, dim).reshape(shape)


def gather_axes(shard, axes, dim):
    far, near = axes
    leading = sent_to_all(shard, far)
    tiles = jnp.swapaxes(sent_to_all(leading, near), 0, 1)
    return in_order(tiles.reshape(-1, *shard.shape), dim)


def nested_sum(shard, axes):
    lines = shard.reshape(-1, shard.shape[-1])
    own = summed_rows(padded_to(lines, lax.axis_size(axes[0]) * lax.axis_size(axes[1])), axes, 0)
    whole = gather_axes(own, axes, 0)
    return whole[: len(lines)].reshape(shard.shape)


def selector(block_sizes, count, width):
    offsets = jnp.cumsum(block_sizes) - block_sizes
    place = jnp.arange(16 * ROWS, dtype=jnp.int32)
    column = jnp.where(place % ROWS < 30, place // ROWS * 30 + place % ROWS, -1)[:, None, None]
    inside = jnp.arange(width, dtype=jnp.int32)[None, None, :]
    hit = (column == offsets[None, :, None] + inside) & (inside < block_sizes[None, :, None])
    return hit.astype(jnp.bfloat16).reshape(16 * ROWS, count * width)


def subspace(cover, block_sizes, keep_count, start_block):
    width = cover.shape[1]
    ranks = start_block.shape[2]
    inside = jnp.arange(width, dtype=jnp.int32)[None, :, None] < block_sizes[:, None, None]
    keep = jnp.minimum(keep_count, (block_sizes + 1) // 2)
    current = jnp.where(inside, start_block, jnp.zeros_like(start_block))
    for turn in range(ITERS):
        product = jnp.einsum("bij,bjk->bik", cover, current, precision=HIGH)
        columns = []
        for column_id in range(ranks):
            vector = product[:, :, column_id]
            for earlier in columns:
                vector = vector - jnp.sum(earlier * vector, axis=1, keepdims=True) * earlier
            length = jnp.sqrt(jnp.sum(vector * vector, axis=1, keepdims=True))
            alive = (column_id < keep)[:, None]
            columns.append(jnp.where(alive, vector / length, jnp.zeros_like(vector)))
        current = jnp.stack(columns, axis=2)
    product = jnp.einsum("bij,bjk->bik", cover, current, precision=HIGH)
    found = jnp.sum(current * product, axis=1)
    return (current, found)


def per_device(images, expansion_basis, block_sizes, keep_count, start_block):
    rows = images.shape[0]
    coeffs = gathered_coeffs(images, expansion_basis)
    samples = coeffs.reshape(2 * rows, 16 * ROWS)
    pick = selector(block_sizes, L, NMAX)
    padded = jnp.dot(samples, pick, preferred_element_type=jnp.float32).astype(jnp.bfloat16)
    wide = padded.reshape(2 * rows, L, NMAX)
    scale = 1.0 / (2 * rows * lax.axis_size(IMG) * lax.axis_size("grp"))
    partial_value = (
        jnp.einsum("rli,rlj->lij", wide, wide, preferred_element_type=jnp.float32) * scale
    )
    cover = nested_sum(partial_value, (("img_0", "img_1"), ("img_2", "grp")))
    vectors, found = subspace(cover, block_sizes, keep_count, start_block)
    rounded = vectors.astype(jnp.bfloat16)
    features = jnp.einsum("rli,lij->rlj", wide, rounded, preferred_element_type=jnp.float32)
    return (features.reshape(rows, 2 * L * KMAX), found)


def solution(mesh):
    split = Mesh(
        mesh.devices.reshape(4, 4, 2, mesh.shape["grp"]), ("img_0", "img_1", "img_2", "grp")
    )
    in_specs = (P(IMG_GRP, None), P(None, IMG), P(), P(), P())
    out_specs = (P(IMG_GRP, None), P())
    return jax.shard_map(
        per_device, mesh=split, in_specs=in_specs, out_specs=out_specs, check_vma=False
    )
```

```python
import functools
import heapq

import jax
import jax.numpy as jnp
from jax import lax
from jax.experimental import pallas as pl
from jax.experimental.pallas import tpu as pltpu
from jax.sharding import Mesh
from jax.sharding import PartitionSpec as P

NMAX = 80
L = 16
S = 480
KMAX = 8
ITERS = 3
AXES = ("img_0", "img_1", "img_2", "grp")
IMG = AXES[:3]
HIGH = lax.Precision.HIGHEST
MESH = pl.DeviceIdType.MESH

KC = 256
SUBS = 4
ROUNDS = 6
CHUNKS = 16 + (ROUNDS - 1) * SUBS
ROWS = 32
BLOCK = ROWS * KC * 2
PART = 16 * ROWS
WIN = 96


class Plan:
    def __init__(self, ahead=2, rate=44e3, hop=1.9, d_rate=500e3, d_hop=1.1, dot=0.3):
        self.program = []
        self.sems = {}
        busy = {}
        now = 0.0
        heap = []
        arrived = {}
        ready = []

        def send(key, link, size):
            sem = self.sems.setdefault(key, len(self.sems))
            fast = link == "d"
            begin = max(busy.get(link, 0.0), now)
            end = begin + size / (d_rate if fast else rate)
            busy[link] = end
            heapq.heappush(heap, (end + (d_hop if fast else hop), sem, key))
            self.program.append(("send", key))

        def axes(sub):
            return ("y", "z") if sub < 2 else ("z", "y")

        def way(sub):
            return ("+", "-") if sub % 2 == 0 else ("-", "+")

        def start_round(r):
            for sub in range(SUBS):
                a = axes(sub)[0]
                send(("1", r, sub, 0), a + "+", BLOCK)
                send(("1", r, sub, 1), a + "-", BLOCK)

        def spread(kind, rest, axis, sub, size):
            send((kind, *rest, 0), axis + "+", size)
            send((kind, *rest, 1), axis + "-", size)

        def got(group, need):
            arrived[group] = arrived.get(group, 0) + 1
            return arrived[group] == need

        def half_done(chunk):
            send(("D", chunk), "d", 16 * BLOCK)
            if got(("C", chunk), 2):
                ready.append(chunk)

        started = 0
        while started < min(ahead, ROUNDS):
            start_round(started)
            started += 1
        while heap or ready:
            if ready and (not heap or heap[0][0] > now or len(ready) > 3):
                chunk = ready.pop(0)
                self.program.append(("dot", chunk))
                now += dot
                continue
            when, _, key = heapq.heappop(heap)
            now = max(now, when) + 0.02
            self.program.append(("wait", key))
            kind = key[0]
            if kind in ("1", "2"):
                _, r, sub, j = key
                axis = axes(sub)[0 if kind == "1" else 1]
                size = BLOCK if kind == "1" else 4 * BLOCK
                if j == sub % 2:
                    send((kind, r, sub, 2), axis + way(sub)[0], size)
                if kind == "1" and got(("1", r, sub), 3):
                    spread("2", (r, sub), axes(sub)[1], sub, 4 * BLOCK)
                    if r == 0:
                        spread("X", (sub, 0), "x", sub, 4 * BLOCK)
                    if sub == SUBS - 1 and started < ROUNDS:
                        start_round(started)
                        started += 1
                if kind == "2":
                    if r == 0:
                        spread("X", (sub, 1 + j), "x", sub, 4 * BLOCK)
                    if got(("2", r, sub), 3):
                        half_done(("own", sub) if r == 0 else ("all", r, sub))
            elif kind == "X":
                _, sub, piece, j = key
                if j == sub % 2:
                    send(("X", sub, piece, 2), "x" + way(sub)[0], 4 * BLOCK)
                if got(("X", sub, j), 4):
                    half_done(("far", j, sub))
            else:
                if got(("C", key[1]), 2):
                    ready.append(key[1])
        self.end = now


def turn(v, by):
    return lax.rem(v + (by + 4), 4)


def device(axis, by):
    spot = dict(zip("yzcx", (lax.axis_index(a) for a in AXES)))
    spot[axis] = turn(spot[axis], by)
    return tuple(spot[a] for a in "yzcx")


def gather_dot(plan, images, own, coeffs, held, pixels, total, fill_sem, send_sem, recv_sem):
    y, z, c, x = (lax.axis_index(a) for a in AXES)
    sibling = (y, z, 1 - c, x)
    barrier = pltpu.get_barrier_semaphore()
    fills = [
        pltpu.make_async_copy(own.at[pl.ds(4 * x, 4)], held.at[pl.ds(4 * x, 4), y, z, c], fill_sem.at[0]),
        pltpu.make_async_copy(own.at[pl.ds(16, CHUNKS - 16)], held.at[pl.ds(16, CHUNKS - 16), y, z, c], fill_sem.at[1]),
        pltpu.make_async_copy(images, pixels, fill_sem.at[2]),
    ]
    for fill in fills:
        fill.start()
    for peer in [device(axis, by) for axis in "yzx" for by in (1, -1)] + [sibling]:
        pl.semaphore_signal(barrier, inc=1, device_id=peer, device_id_type=MESH)
    total[...] = jnp.zeros_like(total)
    pl.semaphore_wait(barrier, 7)
    fills[0].wait()
    fills[1].wait()

    SHIFT = (-1, 1, 2)

    def index(chunk):
        if chunk[0] == "own":
            return 4 * x + chunk[1]
        if chunk[0] == "far":
            return 4 * turn(x, SHIFT[chunk[1]]) + chunk[2]
        return 16 + (chunk[1] - 1) * SUBS + chunk[2]

    def copy_of(key):
        kind = key[0]
        if kind == "D":
            part = held.at[index(key[1]), :, :, c]
            where = sibling
        else:
            j = key[-1]
            sub = key[2] if kind != "X" else key[1]
            step = (1, -1)[j] if j < 2 else (1, -1)[sub % 2]
            back = 0 if j < 2 else -step
            first = sub < 2
            if kind == "1":
                k = index(("own", sub) if key[1] == 0 else ("all", key[1], sub))
                part = held.at[k, turn(y, back), z, c] if first else held.at[k, y, turn(z, back), c]
                where = device("y" if first else "z", step)
            elif kind == "2":
                k = index(("own", sub) if key[1] == 0 else ("all", key[1], sub))
                part = held.at[k, :, turn(z, back), c] if first else held.at[k, turn(y, back), :, c]
                where = device("z" if first else "y", step)
            else:
                k = 4 * turn(x, back) + sub
                shift = (0, *SHIFT)[key[2]]
                if key[2] == 3:
                    shift = 2
                part = held.at[k, :, turn(z, shift), c] if first else held.at[k, turn(y, shift), :, c]
                where = device("x", step)
        sem = plan.sems[key]
        return pltpu.make_async_remote_copy(
            src_ref=part, dst_ref=part, send_sem=send_sem, recv_sem=recv_sem.at[sem],
            device_id=where, device_id_type=MESH,
        )

    sent = []
    loaded = False
    for op, what in plan.program:
        if op == "send":
            copy = copy_of(what)
            copy.start()
            sent.append(copy)
        elif op == "wait":
            copy_of(what).wait_recv()
        else:
            if not loaded:
                fills[2].wait()
                loaded = True
            k = index(what)
            block = held[k].reshape(32 * ROWS, KC)
            rows = pixels[:, pl.ds(pl.multiple_of(k * KC, KC), KC)]
            total[...] += lax.dot_general(
                rows, block, (((1,), (1,)), ((), ())), preferred_element_type=jnp.float32
            )
    for copy in sent:
        copy.wait_send()
    coeffs[...] = total[...].astype(coeffs.dtype)


def places(sizes):
    offsets, firsts = [], []
    offset = jnp.int32(0)
    for l in range(L):
        offsets.append(offset)
        place = lax.div(offset, 30) * ROWS + lax.rem(offset, 30)
        firsts.append(jnp.minimum(lax.div(place, 8) * 8, PART - WIN))
        offset = offset + sizes[l]
    return offsets, firsts


def cut_windows(sizes, keeps, coeffs, start, packed, begin, gram):
    def part_gram(p):
        some = coeffs[:, p * PART : (p + 1) * PART]
        return lax.dot_general(some, some, (((0,), (0,)), ((), ())), preferred_element_type=jnp.float32)

    gram[...] = part_gram(0) + part_gram(1)

    offsets, firsts = places(sizes)

    def window(l):
        left = jnp.minimum(lax.div(firsts[l], 128), 2) * 128
        rows = gram[pl.ds(pl.multiple_of(firsts[l], 8), WIN), pl.ds(pl.multiple_of(left, 128), 256)]
        return pltpu.roll(rows, lax.rem(256 - (firsts[l] - left), 256), 1)[:, :128]

    lane = lax.broadcasted_iota(jnp.int32, (32, 128), 1)
    for pair in range(L // 2):
        one, two = window(2 * pair), window(2 * pair + 1)
        xo, co = pair // 2, pair % 2
        packed[xo, co, 0] = jnp.where(lane < 96, one[:32], pltpu.roll(one[64:], 32, 1))
        packed[xo, co, 1] = jnp.where(lane < 96, two[:32], pltpu.roll(two[64:], 32, 1))
        packed[xo, co, 2] = jnp.where(lane < 64, pltpu.roll(one[32:64], 96, 1), pltpu.roll(two[32:64], 32, 1))

    row = lax.broadcasted_iota(jnp.int32, (KMAX, 128), 0)
    place = lax.broadcasted_iota(jnp.int32, (NMAX, 128), 1)
    inner = lax.broadcasted_iota(jnp.int32, (NMAX, 128), 0)
    for l in range(L):
        slot = lax.rem(firsts[l] + place, ROWS)
        source = lax.div(firsts[l] + place, ROWS) * 30 + slot - offsets[l]
        source = jnp.where(slot < 30, source, -1)
        hit = ((source == inner) & (inner < sizes[l])).astype(jnp.float32)
        lines = slice(KMAX * l, KMAX * l + KMAX)
        begin[0, lines] = jnp.dot(start[l], hit, precision=HIGH, preferred_element_type=jnp.float32)
        begin[1, lines] = jnp.broadcast_to(jnp.sum(hit, axis=0, keepdims=True), (KMAX, 128))
        keep = jnp.minimum(keeps[l], lax.div(sizes[l] + 1, 2))
        begin[2, lines] = (row < keep).astype(jnp.float32)


def iterate(summed, current, inside, alive):
    wide = lax.broadcasted_iota(jnp.int32, (128, 128), 1)
    block_row = lax.div(lax.broadcasted_iota(jnp.int32, (128, 128), 0), 32) * 32

    def cover_of(i):
        low = jnp.zeros((32, 128), jnp.float32)
        middle = pltpu.roll(summed[2], 32 if i == 0 else 96, 1)
        upper = jnp.concatenate([summed[i], middle, pltpu.roll(summed[i], 96, 1), low], axis=0)
        upper = jnp.where((wide >= block_row) & (wide < WIN), upper, 0.0)
        beyond = jnp.where(wide >= block_row + 32, upper, 0.0)
        return upper + beyond.T

    row = lax.broadcasted_iota(jnp.int32, (KMAX, 128), 0)
    column = lax.broadcasted_iota(jnp.int32, (KMAX, 128), 1)

    def times(current, cover):
        return jnp.dot(current, cover, precision=HIGH, preferred_element_type=jnp.float32)

    covers = [cover_of(i) for i in range(2)]
    lines = [slice(KMAX * i, KMAX * i + KMAX) for i in range(2)]
    currents = [current[i] for i in lines]
    inside = [inside[i] > 0.5 for i in lines]
    alive = [alive[i] > 0.5 for i in lines]
    for turn_id in range(ITERS):
        stacks = [jnp.where(inside[i], times(currents[i], covers[i]), 0.0) for i in range(2)]
        norms = [jnp.ones((KMAX, 1), jnp.float32) for _ in range(2)]
        for m in range(KMAX):
            for i in range(2):
                vector = stacks[i][m : m + 1]
                dots = jnp.sum(stacks[i] * vector, axis=1, keepdims=True)
                square = dots[m : m + 1]
                norms[i] = jnp.where(row[:, :1] == m, square, norms[i])
                if m < KMAX - 1:
                    stacks[i] = jnp.where(row > m, stacks[i] - dots / square * vector, stacks[i])
        currents = [jnp.where(alive[i], stacks[i] / jnp.sqrt(norms[i]), 0.0) for i in range(2)]
    ends = []
    for i in range(2):
        quotient = jnp.sum(currents[i] * times(currents[i], covers[i]), axis=1, keepdims=True)
        ends.append(jnp.where(column == 127, quotient, currents[i]))
    return jnp.concatenate(ends, axis=0)


def reduce_iterate(
    scale, packed, begin, everything, half, mate, by_x, by_y, by_z, found, mate_sem, far_sem, found_sem
):
    y, z, c, x = (lax.axis_index(a) for a in AXES)
    sibling = (y, z, 1 - c, x)
    owners = [device("x", by) for by in (1, 2, 3)] + [(y, z, 1 - c, turn(x, by)) for by in range(4)]
    others = [device(axis, by) for axis in "yz" for by in (1, 2, 3)]
    barrier = pltpu.get_barrier_semaphore()
    for peer in owners + others:
        pl.semaphore_signal(barrier, inc=1, device_id=peer, device_id_type=MESH)
    pl.semaphore_wait(barrier, 13)

    def push(src, dst, send, recv, where):
        copy = pltpu.make_async_remote_copy(
            src_ref=src, dst_ref=dst, send_sem=send, recv_sem=recv, device_id=where, device_id_type=MESH
        )
        copy.start()
        return copy

    copy = push(packed.at[:, 1 - c], mate, mate_sem.at[0], mate_sem.at[1], sibling)
    copy.wait()
    for xo in range(4):
        half[xo] = packed[xo, c] + mate[xo]
    copies = [
        push(half.at[turn(x, by)], by_x.at[by - 1], far_sem.at[0, by - 1], far_sem.at[1, by - 1], device("x", by))
        for by in (1, 2, 3)
    ]
    for copy in copies:
        copy.wait()
    by_y[y] = half[x] + by_x[0] + by_x[1] + by_x[2]
    copies = [
        push(by_y.at[y], by_y.at[y], far_sem.at[2, by - 1], far_sem.at[3, by - 1], device("y", by)) for by in (1, 2, 3)
    ]
    for copy in copies:
        copy.wait()
    by_z[z] = by_y[0] + by_y[1] + by_y[2] + by_y[3]
    copies = [
        push(by_z.at[z], by_z.at[z], far_sem.at[4, by - 1], far_sem.at[5, by - 1], device("z", by)) for by in (1, 2, 3)
    ]
    for copy in copies:
        copy.wait()
    me = 2 * x + c
    lines = pl.ds(pl.multiple_of(2 * KMAX * me, 2 * KMAX), 2 * KMAX)
    found[me] = iterate(
        (by_z[0] + by_z[1] + by_z[2] + by_z[3]) * scale, begin[0, lines], begin[1, lines], begin[2, lines]
    )
    copies = [
        push(found.at[me], found.at[me], found_sem.at[0, e], found_sem.at[1, e], owners[e]) for e in range(7)
    ]
    for copy in copies:
        copy.wait()

    everything[...] = found[...].reshape(L * KMAX, 128)


def project(sizes, coeffs, everything, features, values):
    firsts = places(sizes)[1]
    tall = lax.broadcasted_iota(jnp.int32, (L * KMAX, 128), 0)
    wide = lax.broadcasted_iota(jnp.int32, (L * KMAX, 128), 1)
    spread = jnp.where(lax.rem(tall, KMAX) == wide, everything[:, 127:128], 0.0)
    choose = lax.div(lax.broadcasted_iota(jnp.int32, (L, 128), 1), KMAX) == lax.broadcasted_iota(jnp.int32, (L, 128), 0)
    values[...] = jnp.dot(
        choose.astype(jnp.float32), spread, precision=HIGH, preferred_element_type=jnp.float32
    )[:, :KMAX]
    lines = []
    for l in range(L):
        line = jnp.where(wide[:KMAX] < WIN, everything[KMAX * l : KMAX * l + KMAX], 0.0)
        line = jnp.concatenate([line, jnp.zeros((KMAX, PART - 128), jnp.float32)], axis=1)
        lines.append(pltpu.roll(line, firsts[l], 1))
    rounded = jnp.concatenate(lines, axis=0).astype(jnp.bfloat16)
    for p in range(2):
        features[:, p * 128 : (p + 1) * 128] = lax.dot_general(
            coeffs[:, p * PART : (p + 1) * PART], rounded, (((1,), (1,)), ((), ())),
            preferred_element_type=jnp.float32,
        )


def per_device(images, expansion_basis, block_sizes, keep_count, start_block):
    plan = Plan()
    rows = images.shape[0]
    scale = 1.0 / (2 * rows * 128)
    own = jnp.pad(expansion_basis.T, ((0, ROWS - expansion_basis.shape[1]), (0, 0)))
    own = own.reshape(ROWS, CHUNKS, KC).swapaxes(0, 1)
    any_ = pl.BlockSpec(memory_space=pl.ANY)
    scalars = pl.BlockSpec(memory_space=pltpu.SMEM)
    vmem = pl.BlockSpec(memory_space=pltpu.VMEM)
    tiles = (3, 32, 128)
    f32 = jnp.float32
    coeffs = pl.pallas_call(
        functools.partial(gather_dot, plan),
        out_shape=jax.ShapeDtypeStruct((rows, 2 * PART), jnp.bfloat16),
        in_specs=[any_, any_],
        out_specs=vmem,
        scratch_shapes=[
            pltpu.VMEM((CHUNKS, 4, 4, 2, ROWS, KC), jnp.bfloat16),
            pltpu.VMEM(images.shape, jnp.bfloat16),
            pltpu.VMEM((rows, 2 * PART), f32),
            pltpu.SemaphoreType.DMA((3,)),
            pltpu.SemaphoreType.DMA,
            pltpu.SemaphoreType.DMA((len(plan.sems),)),
        ],
        compiler_params=pltpu.CompilerParams(
            collective_id=0, has_side_effects=True, vmem_limit_bytes=58 * 1024 * 1024
        ),
    )(images, own)
    packed, begin = pl.pallas_call(
        cut_windows,
        out_shape=(jax.ShapeDtypeStruct((4, 2, *tiles), f32), jax.ShapeDtypeStruct((3, L * KMAX, 128), f32)),
        in_specs=[scalars, scalars, vmem, vmem],
        out_specs=(vmem, vmem),
        scratch_shapes=[pltpu.VMEM((PART, PART), f32)],
        compiler_params=pltpu.CompilerParams(vmem_limit_bytes=16 * 1024 * 1024),
    )(block_sizes, keep_count, coeffs, start_block.swapaxes(1, 2))
    everything = pl.pallas_call(
        functools.partial(reduce_iterate, scale),
        out_shape=jax.ShapeDtypeStruct((L * KMAX, 128), f32),
        in_specs=[vmem, vmem],
        out_specs=vmem,
        scratch_shapes=[
            pltpu.VMEM((4, *tiles), f32),
            pltpu.VMEM((4, *tiles), f32),
            pltpu.VMEM((3, *tiles), f32),
            pltpu.VMEM((4, *tiles), f32),
            pltpu.VMEM((4, *tiles), f32),
            pltpu.VMEM((8, 2 * KMAX, 128), f32),
            pltpu.SemaphoreType.DMA((2,)),
            pltpu.SemaphoreType.DMA((6, 3)),
            pltpu.SemaphoreType.DMA((2, 7)),
        ],
        compiler_params=pltpu.CompilerParams(
            collective_id=1, has_side_effects=True, vmem_limit_bytes=16 * 1024 * 1024
        ),
    )(packed, begin)
    return pl.pallas_call(
        project,
        out_shape=(
            jax.ShapeDtypeStruct((rows, 2 * L * KMAX), f32),
            jax.ShapeDtypeStruct((L, KMAX), f32),
        ),
        in_specs=[scalars, vmem, vmem],
        out_specs=(vmem, vmem),
        compiler_params=pltpu.CompilerParams(vmem_limit_bytes=16 * 1024 * 1024),
    )(block_sizes, coeffs, everything)


def solution(mesh):
    split = Mesh(mesh.devices.reshape(4, 4, 2, mesh.shape["grp"]), AXES)
    in_specs = (P(AXES, None), P(None, IMG), P(), P(), P())
    out_specs = (P(AXES, None), P())
    return jax.shard_map(
        per_device, mesh=split, in_specs=in_specs, out_specs=out_specs, check_vma=False
    )
```

```python
import functools
import heapq

import jax
import jax.numpy as jnp
from jax import lax
from jax.experimental import pallas as pl
from jax.experimental.pallas import tpu as pltpu
from jax.sharding import Mesh
from jax.sharding import PartitionSpec as P

NMAX = 80
L = 16
S = 480
KMAX = 8
ITERS = 3
AXES = ("img_0", "img_1", "img_2", "grp")
IMG = AXES[:3]
HIGH = lax.Precision.HIGHEST
MESH = pl.DeviceIdType.MESH

KC = 256
SUBS = 4
SIZES = (1, 2, 1, 1, 1)
CHUNKS = 36
ROWS = 32
BLOCK = ROWS * KC * 2
PART = 16 * ROWS
WIN = 96


class Plan:
    def __init__(
        self, window=2.5, late=0.3, turns=0.5, rate=42.5e3, hop=2.8, d_rate=600e3, d_hop=1.4, dot=0.25, queue=3
    ):
        self.program = []
        self.sems = {}
        self.now = 0.0
        busy, pending, arrived = {}, {}, {}
        heap, ready = [], []
        count = iter(range(10**6))

        def to_go(key):
            r, sub, da, db, dx = key
            forward = -1 if sub % 2 == 0 else 1
            if dx:
                return 1 if dx == forward else 0
            hops = 2 if r == 0 else 0
            if db == 0:
                return hops + 2 + (da == forward)
            return hops + (db == forward)

        def issue(key, link, size):
            sem = self.sems.setdefault(key, len(self.sems))
            end = max(busy.get(link, 0.0), self.now) + size / (d_rate if link == "d" else rate)
            busy[link] = end
            heapq.heappush(heap, (end + (d_hop if link == "d" else hop), sem, key))
            self.program.append(("send", key))

        def pump():
            for link, line in pending.items():
                while line and busy.get(link, 0.0) < self.now + window:
                    _, _, key, size = heapq.heappop(line)
                    issue(key, link, size)

        def along(axis, place, at, key):
            forward = -1 if key[1] % 2 == 0 else 1
            if place == 0:
                steps = ((-1, "+"), (1, "-"))
            elif place == forward:
                steps = ((2, "+" if forward == -1 else "-"),)
            else:
                steps = ()
            for there, sign in steps:
                onto = key[:at] + (there,) + key[at + 1 :]
                rank = onto[0] * late + onto[1] * turns - to_go(onto)
                line = pending.setdefault(axis + sign, [])
                heapq.heappush(line, (rank, next(count), onto, SIZES[key[0]] * BLOCK))

        def onward(key):
            r, sub, da, db, dx = key
            first, second = ("y", "z") if sub < 2 else ("z", "y")
            if dx == 0:
                if db == 0:
                    along(first, da, 2, key)
                along(second, db, 3, key)
            if r == 0 and (da, db) != (0, 0):
                along("x", dx, 4, key)

        def got(group, need):
            arrived[group] = arrived.get(group, 0) + 1
            return arrived[group] == need

        for r in range(len(SIZES)):
            for sub in range(SUBS):
                onward((r, sub, 0, 0, 0))
        pump()
        while heap or ready:
            if ready and (not heap or heap[0][0] > self.now or len(ready) > queue):
                self.program.append(("dot", ready.pop(0)))
                self.now += dot
            else:
                when, _, key = heapq.heappop(heap)
                self.now = max(self.now, when) + 0.02
                self.program.append(("wait", key))
                if key[0] == "D":
                    chunk = key[1:4]
                else:
                    onward(key)
                    chunk = (key[0], key[1], key[4])
                    if got((*chunk, "line", key[3]), 4 if key[3] else 3):
                        issue(("D", *chunk, key[3]), "d", 4 * BLOCK * SIZES[key[0]])
                if got(chunk, 19):
                    ready.extend((*chunk, k) for k in range(SIZES[chunk[0]]))
            pump()
        self.end = self.now


def turn(v, by):
    return lax.rem(v + (by + 4), 4)


def device(axis, by):
    spot = dict(zip("yzcx", (lax.axis_index(a) for a in AXES)))
    spot[axis] = turn(spot[axis], by)
    return tuple(spot[a] for a in "yzcx")


def gather_dot(plan, images, basis, coeffs, held, pixels, total, fill_sem, send_sem, recv_sem):
    y, z, c, x = (lax.axis_index(a) for a in AXES)
    sibling = (y, z, 1 - c, x)
    barrier = pltpu.get_barrier_semaphore()
    for peer in [device(axis, by) for axis in "yzx" for by in (1, -1)] + [sibling]:
        pl.semaphore_signal(barrier, inc=1, device_id=peer, device_id_type=MESH)
    fill = pltpu.make_async_copy(images, pixels, fill_sem)
    fill.start()
    for k in range(CHUNKS):
        held[k, y, z, c] = jnp.zeros((ROWS, KC), jnp.bfloat16)
        held[k, y, z, c, : basis.shape[0]] = basis[:, k * KC : (k + 1) * KC]
    total[...] = jnp.zeros_like(total)
    pl.semaphore_wait(barrier, 7)

    def index(r, sub, dx):
        if r == 0:
            return SUBS * turn(x, dx) + sub
        return SUBS * (4 + sum(SIZES[1:r])) + sub * SIZES[r]

    def copy_of(key):
        if key[0] == "D":
            r, sub, dx, db = key[1:]
            k = pl.ds(index(r, sub, dx), SIZES[r])
            part = held.at[k, :, turn(z, db), c] if sub < 2 else held.at[k, turn(y, db), :, c]
            where = sibling
        else:
            r, sub = key[:2]
            place = list(key[2:])
            moving = 2 if place[2] else 1 if place[1] else 0
            forward = -1 if sub % 2 == 0 else 1
            there = place[moving]
            step = -there if there != 2 else -forward
            place[moving] = 0 if there != 2 else forward
            da, db, dx = place
            dy, dz = (da, db) if sub < 2 else (db, da)
            part = held.at[pl.ds(index(r, sub, dx), SIZES[r]), turn(y, dy), turn(z, dz), c]
            where = device(("yzx" if sub < 2 else "zyx")[moving], step)
        return pltpu.make_async_remote_copy(
            src_ref=part, dst_ref=part, send_sem=send_sem, recv_sem=recv_sem.at[plan.sems[key]],
            device_id=where, device_id_type=MESH,
        )

    sent = []
    loaded = False
    for op, what in plan.program:
        if op == "send":
            copy = copy_of(what)
            copy.start()
            sent.append(copy)
        elif op == "wait":
            copy_of(what).wait_recv()
        else:
            if not loaded:
                fill.wait()
                loaded = True
            k = index(*what[:3]) + what[3]
            block = held[k].reshape(32 * ROWS, KC)
            rows = pixels[:, pl.ds(pl.multiple_of(k * KC, KC), KC)]
            total[...] += lax.dot_general(
                rows, block, (((1,), (1,)), ((), ())), preferred_element_type=jnp.float32
            )
    if not loaded:
        fill.wait()
    for copy in sent:
        copy.wait_send()
    coeffs[...] = total[...].astype(coeffs.dtype)


def places(sizes):
    offsets, firsts = [], []
    offset = jnp.int32(0)
    for l in range(L):
        offsets.append(offset)
        place = lax.div(offset, 30) * ROWS + lax.rem(offset, 30)
        firsts.append(jnp.minimum(lax.div(place, 8) * 8, PART - WIN))
        offset = offset + sizes[l]
    return offsets, firsts


def cut_windows(sizes, keeps, coeffs, start, packed, begin, gram):
    def part_gram(p):
        some = coeffs[:, p * PART : (p + 1) * PART]
        return lax.dot_general(some, some, (((0,), (0,)), ((), ())), preferred_element_type=jnp.float32)

    gram[...] = part_gram(0) + part_gram(1)

    offsets, firsts = places(sizes)

    def window(l):
        left = jnp.minimum(lax.div(firsts[l], 128), 2) * 128
        rows = gram[pl.ds(pl.multiple_of(firsts[l], 8), WIN), pl.ds(pl.multiple_of(left, 128), 256)]
        return pltpu.roll(rows, lax.rem(256 - (firsts[l] - left), 256), 1)[:, :128]

    lane = lax.broadcasted_iota(jnp.int32, (32, 128), 1)
    for pair in range(L // 2):
        one, two = window(2 * pair), window(2 * pair + 1)
        xo, co = pair // 2, pair % 2
        packed[xo, co, 0] = jnp.where(lane < 96, one[:32], pltpu.roll(one[64:], 32, 1))
        packed[xo, co, 1] = jnp.where(lane < 96, two[:32], pltpu.roll(two[64:], 32, 1))
        packed[xo, co, 2] = jnp.where(lane < 64, pltpu.roll(one[32:64], 96, 1), pltpu.roll(two[32:64], 32, 1))

    row = lax.broadcasted_iota(jnp.int32, (KMAX, 128), 0)
    place = lax.broadcasted_iota(jnp.int32, (NMAX, 128), 1)
    inner = lax.broadcasted_iota(jnp.int32, (NMAX, 128), 0)
    for l in range(L):
        slot = lax.rem(firsts[l] + place, ROWS)
        source = lax.div(firsts[l] + place, ROWS) * 30 + slot - offsets[l]
        source = jnp.where(slot < 30, source, -1)
        hit = ((source == inner) & (inner < sizes[l])).astype(jnp.float32)
        lines = slice(KMAX * l, KMAX * l + KMAX)
        begin[0, lines] = jnp.dot(start[l], hit, precision=HIGH, preferred_element_type=jnp.float32)
        begin[1, lines] = jnp.broadcast_to(jnp.sum(hit, axis=0, keepdims=True), (KMAX, 128))
        keep = jnp.minimum(keeps[l], lax.div(sizes[l] + 1, 2))
        begin[2, lines] = (row < keep).astype(jnp.float32)


def iterate(summed, current, inside, alive):
    wide = lax.broadcasted_iota(jnp.int32, (128, 128), 1)
    block_row = lax.div(lax.broadcasted_iota(jnp.int32, (128, 128), 0), 32) * 32

    def cover_of(i):
        low = jnp.zeros((32, 128), jnp.float32)
        middle = pltpu.roll(summed[2], 32 if i == 0 else 96, 1)
        upper = jnp.concatenate([summed[i], middle, pltpu.roll(summed[i], 96, 1), low], axis=0)
        upper = jnp.where((wide >= block_row) & (wide < WIN), upper, 0.0)
        beyond = jnp.where(wide >= block_row + 32, upper, 0.0)
        return upper + beyond.T

    row = lax.broadcasted_iota(jnp.int32, (KMAX, 128), 0)
    column = lax.broadcasted_iota(jnp.int32, (KMAX, 128), 1)

    def times(current, cover):
        return jnp.dot(current, cover, precision=HIGH, preferred_element_type=jnp.float32)

    covers = [cover_of(i) for i in range(2)]
    lines = [slice(KMAX * i, KMAX * i + KMAX) for i in range(2)]
    currents = [current[i] for i in lines]
    inside = [inside[i] > 0.5 for i in lines]
    alive = [alive[i] > 0.5 for i in lines]
    for turn_id in range(ITERS):
        stacks = [jnp.where(inside[i], times(currents[i], covers[i]), 0.0) for i in range(2)]
        norms = [jnp.ones((KMAX, 1), jnp.float32) for _ in range(2)]
        for m in range(KMAX):
            for i in range(2):
                vector = stacks[i][m : m + 1]
                dots = jnp.sum(stacks[i] * vector, axis=1, keepdims=True)
                square = dots[m : m + 1]
                norms[i] = jnp.where(row[:, :1] == m, square, norms[i])
                if m < KMAX - 1:
                    stacks[i] = jnp.where(row > m, stacks[i] - dots / square * vector, stacks[i])
        currents = [jnp.where(alive[i], stacks[i] / jnp.sqrt(norms[i]), 0.0) for i in range(2)]
    ends = []
    for i in range(2):
        quotient = jnp.sum(currents[i] * times(currents[i], covers[i]), axis=1, keepdims=True)
        ends.append(jnp.where(column == 127, quotient, currents[i]))
    return jnp.concatenate(ends, axis=0)


def reduce_iterate(scale, packed, begin, everything, mate, half, by_x, one, two, found, mate_sem, far_sem, found_sem):
    y, z, c, x = (lax.axis_index(a) for a in AXES)
    sibling = (y, z, 1 - c, x)
    owners = [device("x", by) for by in (1, 2, 3)] + [(y, z, 1 - c, turn(x, by)) for by in range(4)]
    barrier = pltpu.get_barrier_semaphore()
    for peer in owners + [device(axis, by) for axis in "yz" for by in (1, 2, 3)]:
        pl.semaphore_signal(barrier, inc=1, device_id=peer, device_id_type=MESH)
    pl.semaphore_wait(barrier, 13)
    sent = []

    def push(src, dst, sems, where):
        copy = pltpu.make_async_remote_copy(
            src_ref=src, dst_ref=dst, send_sem=sems[0], recv_sem=sems[1], device_id=where, device_id_type=MESH
        )
        copy.start()
        sent.append(copy)
        return copy

    def far(stage, h):
        return [(far_sem.at[stage, h, 0, by - 1], far_sem.at[stage, h, 1, by - 1]) for by in (1, 2, 3)]

    push(packed.at[:, 1 - c], mate, (mate_sem.at[0], mate_sem.at[1]), sibling).wait_recv()
    copies = []
    for h in range(2):
        lines = slice(16 * h, 16 * h + 16)
        for xo in range(4):
            half[h, xo] = packed[xo, c, :, lines] + mate[xo, :, lines]
        copies.append([
            push(half.at[h, turn(x, by)], by_x.at[h, by - 1], far(0, h)[by - 1], device("x", by)) for by in (1, 2, 3)
        ])
    for stage, (land, spots, axes) in enumerate(((one, (y, z), "yz"), (two, (z, y), "zy"))):
        onward = []
        for h in range(2):
            for copy in copies[h]:
                copy.wait_recv()
            spot = spots[h]
            if stage == 0:
                land[h, spot] = half[h, x] + by_x[h, 0] + by_x[h, 1] + by_x[h, 2]
            else:
                land[h, spot] = one[h, 0] + one[h, 1] + one[h, 2] + one[h, 3]
            onward.append([
                push(land.at[h, spot], land.at[h, spot], far(1 + stage, h)[by - 1], device(axes[h], by))
                for by in (1, 2, 3)
            ])
        copies = onward
    for h in range(2):
        for copy in copies[h]:
            copy.wait_recv()
    sums = [two[h, 0] + two[h, 1] + two[h, 2] + two[h, 3] for h in range(2)]
    summed = jnp.concatenate(sums, axis=1) * scale

    me = 2 * x + c
    lines = pl.ds(pl.multiple_of(2 * KMAX * me, 2 * KMAX), 2 * KMAX)
    found[me] = iterate(summed, begin[0, lines], begin[1, lines], begin[2, lines])
    copies = [push(found.at[me], found.at[me], (found_sem.at[0, e], found_sem.at[1, e]), owners[e]) for e in range(7)]
    for copy in copies:
        copy.wait_recv()
    everything[...] = found[...].reshape(L * KMAX, 128)
    for copy in sent:
        copy.wait_send()


def project(sizes, coeffs, everything, features, values):
    firsts = places(sizes)[1]
    tall = lax.broadcasted_iota(jnp.int32, (L * KMAX, 128), 0)
    wide = lax.broadcasted_iota(jnp.int32, (L * KMAX, 128), 1)
    spread = jnp.where(lax.div(tall, KMAX) == wide, everything[:, 127:128], 0.0)
    choose = lax.rem(wide[:KMAX], KMAX) == tall[:KMAX]
    values[...] = jnp.dot(
        choose.astype(jnp.float32), spread, precision=HIGH, preferred_element_type=jnp.float32
    )[:, :L]
    lines = []
    for l in range(L):
        line = jnp.where(wide[:KMAX] < WIN, everything[KMAX * l : KMAX * l + KMAX], 0.0)
        line = jnp.concatenate([line, jnp.zeros((KMAX, PART - 128), jnp.float32)], axis=1)
        lines.append(pltpu.roll(line, firsts[l], 1))
    rounded = jnp.concatenate(lines, axis=0).astype(jnp.bfloat16)
    for p in range(2):
        features[:, p * 128 : (p + 1) * 128] = lax.dot_general(
            coeffs[:, p * PART : (p + 1) * PART], rounded, (((1,), (1,)), ((), ())),
            preferred_element_type=jnp.float32,
        )


def per_device(images, expansion_basis, block_sizes, keep_count, start_block):
    plan = Plan()
    rows = images.shape[0]
    scale = 1.0 / (2 * rows * 128)
    scalars = pl.BlockSpec(memory_space=pltpu.SMEM)
    vmem = pl.BlockSpec(memory_space=pltpu.VMEM)
    f32, bf16 = jnp.float32, jnp.bfloat16
    tiles, halves = (3, 32, 128), (3, 16, 128)
    coeffs = pl.pallas_call(
        functools.partial(gather_dot, plan),
        out_shape=jax.ShapeDtypeStruct((rows, 2 * PART), bf16),
        in_specs=[pl.BlockSpec(memory_space=pltpu.HBM), vmem],
        out_specs=vmem,
        scratch_shapes=[
            pltpu.VMEM((CHUNKS, 4, 4, 2, ROWS, KC), bf16),
            pltpu.VMEM(images.shape, bf16),
            pltpu.VMEM((rows, 2 * PART), f32),
            pltpu.SemaphoreType.DMA,
            pltpu.SemaphoreType.DMA,
            pltpu.SemaphoreType.DMA((len(plan.sems),)),
        ],
        compiler_params=pltpu.CompilerParams(
            collective_id=0, has_side_effects=True, vmem_limit_bytes=52 * 1024 * 1024
        ),
    )(images, expansion_basis.T)
    packed, begin = pl.pallas_call(
        cut_windows,
        out_shape=(jax.ShapeDtypeStruct((4, 2, *tiles), f32), jax.ShapeDtypeStruct((3, L * KMAX, 128), f32)),
        in_specs=[scalars, scalars, vmem, vmem],
        out_specs=(vmem, vmem),
        scratch_shapes=[pltpu.VMEM((PART, PART), f32)],
        compiler_params=pltpu.CompilerParams(vmem_limit_bytes=16 * 1024 * 1024),
    )(block_sizes, keep_count, coeffs, start_block.swapaxes(1, 2))
    everything = pl.pallas_call(
        functools.partial(reduce_iterate, scale),
        out_shape=jax.ShapeDtypeStruct((L * KMAX, 128), f32),
        in_specs=[vmem, vmem],
        out_specs=vmem,
        scratch_shapes=[
            pltpu.VMEM((4, *tiles), f32),
            pltpu.VMEM((2, 4, *halves), f32),
            pltpu.VMEM((2, 3, *halves), f32),
            pltpu.VMEM((2, 4, *halves), f32),
            pltpu.VMEM((2, 4, *halves), f32),
            pltpu.VMEM((8, 2 * KMAX, 128), f32),
            pltpu.SemaphoreType.DMA((2,)),
            pltpu.SemaphoreType.DMA((3, 2, 2, 3)),
            pltpu.SemaphoreType.DMA((2, 7)),
        ],
        compiler_params=pltpu.CompilerParams(
            collective_id=1, has_side_effects=True, vmem_limit_bytes=16 * 1024 * 1024
        ),
    )(packed, begin)
    features, values = pl.pallas_call(
        project,
        out_shape=(
            jax.ShapeDtypeStruct((rows, 2 * L * KMAX), f32),
            jax.ShapeDtypeStruct((KMAX, L), f32),
        ),
        in_specs=[scalars, vmem, vmem],
        out_specs=(vmem, vmem),
        compiler_params=pltpu.CompilerParams(vmem_limit_bytes=16 * 1024 * 1024),
    )(block_sizes, coeffs, everything)
    return features, values.T


def solution(mesh):
    split = Mesh(mesh.devices.reshape(4, 4, 2, mesh.shape["grp"]), AXES)
    in_specs = (P(AXES, None), P(None, IMG), P(), P(), P())
    out_specs = (P(AXES, None), P())
    return jax.shard_map(
        per_device, mesh=split, in_specs=in_specs, out_specs=out_specs, check_vma=False
    )
```

```python
import functools
import heapq

import jax
import jax.numpy as jnp
from jax import lax
from jax.experimental import pallas as pl
from jax.experimental.pallas import tpu as pltpu
from jax.sharding import Mesh
from jax.sharding import PartitionSpec as P

NMAX = 80
L = 16
S = 480
KMAX = 8
ITERS = 3
AXES = ("img_0", "img_1", "img_2", "grp")
IMG = AXES[:3]
HIGH = lax.Precision.HIGHEST
MESH = pl.DeviceIdType.MESH

KC = 256
SUBS = 4
SIZES = (1, 2, 1, 1, 1)
CHUNKS = 36
ROWS = 32
BLOCK = ROWS * KC * 2
PLANE = (-1, 1, -1, 1)
PART = 16 * ROWS
WIN = 96


class Plan:
    def __init__(
        self, window=2.5, late=0.3, turns=0.5, spare=-1.0, rate=42.5e3, hop=2.8, d_rate=600e3, d_hop=1.4, dot=0.25, queue=3
    ):
        self.program = []
        self.sems = {}
        self.now = 0.0
        busy, pending, arrived = {}, {}, {}
        heap, ready = [], []
        count = iter(range(10**6))

        def to_go(key):
            r, sub, da, db, dx = key
            forward = -1 if sub % 2 == 0 else 1
            if dx:
                return 1 if dx == forward else 0
            hops = 2 if r == 0 else 0
            if db == 0:
                return hops + 2 + (da == forward)
            return hops + (db == forward)

        def issue(key, link, size):
            sem = self.sems.setdefault(key, len(self.sems))
            end = max(busy.get(link, 0.0), self.now) + size / (d_rate if link == "d" else rate)
            busy[link] = end
            heapq.heappush(heap, (end + (d_hop if link == "d" else hop), sem, key))
            self.program.append(("send", key))

        def pump():
            for link, line in pending.items():
                while line and busy.get(link, 0.0) < self.now + window:
                    _, _, key, size = heapq.heappop(line)
                    issue(key, link, size)

        def enqueue(link, rank, key):
            heapq.heappush(pending.setdefault(link, []), (rank, next(count), key, SIZES[key[0]] * BLOCK))

        def along(axis, place, at, key):
            forward = -1 if key[1] % 2 == 0 else 1
            if place == 0:
                steps = ((-1, "+"), (1, "-"))
            elif place == forward:
                steps = ((2, "+" if forward == -1 else "-"),)
            else:
                steps = ()
            for there, sign in steps:
                onto = key[:at] + (there,) + key[at + 1 :]
                enqueue(axis + sign, onto[0] * late + onto[1] * turns - to_go(onto), onto)

        def onward(key):
            r, sub, da, db, dx = key
            first, second = ("y", "z") if sub < 2 else ("z", "y")
            if dx == 0:
                if db == 0:
                    along(first, da, 2, key)
                along(second, db, 3, key)
            if r == 0 and (da, db) not in ((0, 0), (PLANE[sub], 0)):
                along("x", dx, 4, key)

        def got(group, need):
            arrived[group] = arrived.get(group, 0) + 1
            return arrived[group] == need

        for r in range(len(SIZES)):
            for sub in range(SUBS):
                onward((r, sub, 0, 0, 0))
        for sub in range(SUBS):
            for dx in (-1, 1, 2):
                if PLANE[sub]:
                    link = ("y" if sub < 2 else "z") + ("+" if PLANE[sub] < 0 else "-")
                    enqueue(link, spare + sub * turns, (0, sub, PLANE[sub], 0, dx))
        pump()
        while heap or ready:
            if ready and (not heap or heap[0][0] > self.now or len(ready) > queue):
                self.program.append(("dot", ready.pop(0)))
                self.now += dot
            else:
                when, _, key = heapq.heappop(heap)
                self.now = max(self.now, when) + 0.02
                self.program.append(("wait", key))
                if key[0] == "D":
                    chunk = key[1:4]
                else:
                    onward(key)
                    chunk = (key[0], key[1], key[4])
                    if got((*chunk, "line", key[3]), 4 if key[3] else 3):
                        issue(("D", *chunk, key[3]), "d", 4 * BLOCK * SIZES[key[0]])
                if got(chunk, 19):
                    ready.extend((*chunk, k) for k in range(SIZES[chunk[0]]))
            pump()
        self.end = self.now


def turn(v, by):
    return lax.rem(v + (by + 4), 4)


def device(axis, by):
    spot = dict(zip("yzcx", (lax.axis_index(a) for a in AXES)))
    spot[axis] = turn(spot[axis], by)
    return tuple(spot[a] for a in "yzcx")


def gather_dot(plan, images, basis, coeffs, held, stage, pixels, total, fill_sem, send_sem, recv_sem):
    y, z, c, x = (lax.axis_index(a) for a in AXES)
    sibling = (y, z, 1 - c, x)
    barrier = pltpu.get_barrier_semaphore()
    own = pltpu.make_async_copy(basis, stage, fill_sem.at[0])
    own.start()
    for peer in [device(axis, by) for axis in "yzx" for by in (1, -1)] + [sibling]:
        pl.semaphore_signal(barrier, inc=1, device_id=peer, device_id_type=MESH)
    total[...] = jnp.zeros_like(total)
    own.wait()
    fill = pltpu.make_async_copy(images, pixels, fill_sem.at[1])
    fill.start()
    for k in range(CHUNKS):
        held[k, y, z, c] = jnp.zeros((ROWS, KC), jnp.bfloat16)
        held[k, y, z, c, : stage.shape[0]] = stage[:, k * KC : (k + 1) * KC]
    pl.semaphore_wait(barrier, 7)

    def index(r, sub, dx):
        if r == 0:
            return SUBS * turn(x, dx) + sub
        return SUBS * (4 + sum(SIZES[1:r])) + sub * SIZES[r]

    def copy_of(key):
        if key[0] == "D":
            r, sub, dx, db = key[1:]
            k = pl.ds(index(r, sub, dx), SIZES[r])
            part = held.at[k, :, turn(z, db), c] if sub < 2 else held.at[k, turn(y, db), :, c]
            where = sibling
        else:
            r, sub = key[:2]
            place = list(key[2:])
            moving = 2 if place[2] and place[:2] != [PLANE[sub], 0] else 1 if place[1] else 0
            forward = -1 if sub % 2 == 0 else 1
            there = place[moving]
            step = -there if there != 2 else -forward
            place[moving] = 0 if there != 2 else forward
            da, db, dx = place
            dy, dz = (da, db) if sub < 2 else (db, da)
            part = held.at[pl.ds(index(r, sub, dx), SIZES[r]), turn(y, dy), turn(z, dz), c]
            where = device(("yzx" if sub < 2 else "zyx")[moving], step)
        return pltpu.make_async_remote_copy(
            src_ref=part, dst_ref=part, send_sem=send_sem, recv_sem=recv_sem.at[plan.sems[key]],
            device_id=where, device_id_type=MESH,
        )

    sent = []
    loaded = False
    for op, what in plan.program:
        if op == "send":
            copy = copy_of(what)
            copy.start()
            sent.append(copy)
        elif op == "wait":
            copy_of(what).wait_recv()
        else:
            if not loaded:
                fill.wait()
                loaded = True
            k = index(*what[:3]) + what[3]
            block = held[k].reshape(32 * ROWS, KC)
            rows = pixels[:, pl.ds(pl.multiple_of(k * KC, KC), KC)]
            total[...] += lax.dot_general(
                rows, block, (((1,), (1,)), ((), ())), preferred_element_type=jnp.float32
            )
    if not loaded:
        fill.wait()
    for copy in sent:
        copy.wait_send()
    coeffs[...] = total[...].astype(coeffs.dtype)


def places(sizes):
    offsets, firsts = [], []
    offset = jnp.int32(0)
    for l in range(L):
        offsets.append(offset)
        place = lax.div(offset, 30) * ROWS + lax.rem(offset, 30)
        firsts.append(jnp.minimum(lax.div(place, 8) * 8, PART - WIN))
        offset = offset + sizes[l]
    return offsets, firsts


def cut_windows(sizes, keeps, coeffs, start, packed, begin, gram):
    def part_gram(p):
        some = coeffs[:, p * PART : (p + 1) * PART]
        return lax.dot_general(some, some, (((0,), (0,)), ((), ())), preferred_element_type=jnp.float32)

    gram[...] = part_gram(0) + part_gram(1)

    offsets, firsts = places(sizes)

    def window(l):
        left = jnp.minimum(lax.div(firsts[l], 128), 2) * 128
        rows = gram[pl.ds(pl.multiple_of(firsts[l], 8), WIN), pl.ds(pl.multiple_of(left, 128), 256)]
        return pltpu.roll(rows, lax.rem(256 - (firsts[l] - left), 256), 1)[:, :128]

    lane = lax.broadcasted_iota(jnp.int32, (32, 128), 1)
    for pair in range(L // 2):
        one, two = window(2 * pair), window(2 * pair + 1)
        xo, co = pair // 2, pair % 2
        packed[xo, co, 0] = jnp.where(lane < 96, one[:32], pltpu.roll(one[64:], 32, 1))
        packed[xo, co, 1] = jnp.where(lane < 96, two[:32], pltpu.roll(two[64:], 32, 1))
        packed[xo, co, 2] = jnp.where(lane < 64, pltpu.roll(one[32:64], 96, 1), pltpu.roll(two[32:64], 32, 1))

    row = lax.broadcasted_iota(jnp.int32, (KMAX, 128), 0)
    place = lax.broadcasted_iota(jnp.int32, (NMAX, 128), 1)
    inner = lax.broadcasted_iota(jnp.int32, (NMAX, 128), 0)
    for l in range(L):
        slot = lax.rem(firsts[l] + place, ROWS)
        source = lax.div(firsts[l] + place, ROWS) * 30 + slot - offsets[l]
        source = jnp.where(slot < 30, source, -1)
        hit = ((source == inner) & (inner < sizes[l])).astype(jnp.float32)
        lines = slice(KMAX * l, KMAX * l + KMAX)
        begin[0, lines] = jnp.dot(start[l], hit, precision=HIGH, preferred_element_type=jnp.float32)
        begin[1, lines] = jnp.broadcast_to(jnp.sum(hit, axis=0, keepdims=True), (KMAX, 128))
        keep = jnp.minimum(keeps[l], lax.div(sizes[l] + 1, 2))
        begin[2, lines] = (row < keep).astype(jnp.float32)


def iterate(summed, current, inside, alive):
    wide = lax.broadcasted_iota(jnp.int32, (128, 128), 1)
    block_row = lax.div(lax.broadcasted_iota(jnp.int32, (128, 128), 0), 32) * 32

    def cover_of(i):
        low = jnp.zeros((32, 128), jnp.float32)
        middle = pltpu.roll(summed[2], 32 if i == 0 else 96, 1)
        upper = jnp.concatenate([summed[i], middle, pltpu.roll(summed[i], 96, 1), low], axis=0)
        upper = jnp.where((wide >= block_row) & (wide < WIN), upper, 0.0)
        beyond = jnp.where(wide >= block_row + 32, upper, 0.0)
        return upper + beyond.T

    row = lax.broadcasted_iota(jnp.int32, (KMAX, 128), 0)
    column = lax.broadcasted_iota(jnp.int32, (KMAX, 128), 1)

    def times(current, cover):
        return jnp.dot(current, cover, precision=HIGH, preferred_element_type=jnp.float32)

    covers = [cover_of(i) for i in range(2)]
    lines = [slice(KMAX * i, KMAX * i + KMAX) for i in range(2)]
    currents = [current[i] for i in lines]
    inside = [inside[i] > 0.5 for i in lines]
    alive = [alive[i] > 0.5 for i in lines]
    for turn_id in range(ITERS):
        stacks = [jnp.where(inside[i], times(currents[i], covers[i]), 0.0) for i in range(2)]
        norms = [jnp.ones((KMAX, 1), jnp.float32) for _ in range(2)]
        for m in range(KMAX):
            for i in range(2):
                vector = stacks[i][m : m + 1]
                dots = jnp.sum(stacks[i] * vector, axis=1, keepdims=True)
                square = dots[m : m + 1]
                norms[i] = jnp.where(row[:, :1] == m, square, norms[i])
                if m < KMAX - 1:
                    stacks[i] = jnp.where(row > m, stacks[i] - dots / square * vector, stacks[i])
        currents = [jnp.where(alive[i], stacks[i] / jnp.sqrt(norms[i]), 0.0) for i in range(2)]
    ends = []
    for i in range(2):
        quotient = jnp.sum(currents[i] * times(currents[i], covers[i]), axis=1, keepdims=True)
        ends.append(jnp.where(column == 127, quotient, currents[i]))
    return jnp.concatenate(ends, axis=0)


def reduce_iterate(scale, packed, begin, everything, mate, half, by_x, one, two, found, mate_sem, far_sem, found_sem):
    y, z, c, x = (lax.axis_index(a) for a in AXES)
    sibling = (y, z, 1 - c, x)
    owners = [device("x", by) for by in (1, 2, 3)] + [(y, z, 1 - c, turn(x, by)) for by in range(4)]
    barrier = pltpu.get_barrier_semaphore()
    for peer in owners + [device(axis, by) for axis in "yz" for by in (1, 2, 3)]:
        pl.semaphore_signal(barrier, inc=1, device_id=peer, device_id_type=MESH)
    pl.semaphore_wait(barrier, 13)
    sent = []

    def push(src, dst, sems, where):
        copy = pltpu.make_async_remote_copy(
            src_ref=src, dst_ref=dst, send_sem=sems[0], recv_sem=sems[1], device_id=where, device_id_type=MESH
        )
        copy.start()
        sent.append(copy)
        return copy

    def far(stage, h):
        return [(far_sem.at[stage, h, 0, by - 1], far_sem.at[stage, h, 1, by - 1]) for by in (1, 2, 3)]

    push(packed.at[:, 1 - c], mate, (mate_sem.at[0], mate_sem.at[1]), sibling).wait_recv()
    copies = []
    for h in range(2):
        lines = slice(16 * h, 16 * h + 16)
        for xo in range(4):
            half[h, xo] = packed[xo, c, :, lines] + mate[xo, :, lines]
        copies.append([
            push(half.at[h, turn(x, by)], by_x.at[h, by - 1], far(0, h)[by - 1], device("x", by)) for by in (1, 2, 3)
        ])
    for stage, (land, spots, axes) in enumerate(((one, (y, z), "yz"), (two, (z, y), "zy"))):
        onward = []
        for h in range(2):
            for copy in copies[h]:
                copy.wait_recv()
            spot = spots[h]
            if stage == 0:
                land[h, spot] = half[h, x] + by_x[h, 0] + by_x[h, 1] + by_x[h, 2]
            else:
                land[h, spot] = one[h, 0] + one[h, 1] + one[h, 2] + one[h, 3]
            onward.append([
                push(land.at[h, spot], land.at[h, spot], far(1 + stage, h)[by - 1], device(axes[h], by))
                for by in (1, 2, 3)
            ])
        copies = onward
    for h in range(2):
        for copy in copies[h]:
            copy.wait_recv()
    sums = [two[h, 0] + two[h, 1] + two[h, 2] + two[h, 3] for h in range(2)]
    summed = jnp.concatenate(sums, axis=1) * scale

    me = 2 * x + c
    lines = pl.ds(pl.multiple_of(2 * KMAX * me, 2 * KMAX), 2 * KMAX)
    found[me] = iterate(summed, begin[0, lines], begin[1, lines], begin[2, lines])
    copies = [push(found.at[me], found.at[me], (found_sem.at[0, e], found_sem.at[1, e]), owners[e]) for e in range(7)]
    for copy in copies:
        copy.wait_recv()
    everything[...] = found[...].reshape(L * KMAX, 128)
    for copy in sent:
        copy.wait_send()


def project(sizes, coeffs, everything, features, values):
    firsts = places(sizes)[1]
    tall = lax.broadcasted_iota(jnp.int32, (L * KMAX, 128), 0)
    wide = lax.broadcasted_iota(jnp.int32, (L * KMAX, 128), 1)
    spread = jnp.where(lax.div(tall, KMAX) == wide, everything[:, 127:128], 0.0)
    choose = lax.rem(wide[:KMAX], KMAX) == tall[:KMAX]
    values[...] = jnp.dot(
        choose.astype(jnp.float32), spread, precision=HIGH, preferred_element_type=jnp.float32
    )[:, :L]
    lines = []
    for l in range(L):
        line = jnp.where(wide[:KMAX] < WIN, everything[KMAX * l : KMAX * l + KMAX], 0.0)
        line = jnp.concatenate([line, jnp.zeros((KMAX, PART - 128), jnp.float32)], axis=1)
        lines.append(pltpu.roll(line, firsts[l], 1))
    rounded = jnp.concatenate(lines, axis=0).astype(jnp.bfloat16)
    for p in range(2):
        features[:, p * 128 : (p + 1) * 128] = lax.dot_general(
            coeffs[:, p * PART : (p + 1) * PART], rounded, (((1,), (1,)), ((), ())),
            preferred_element_type=jnp.float32,
        )


def per_device(images, expansion_basis, block_sizes, keep_count, start_block):
    plan = Plan()
    rows = images.shape[0]
    scale = 1.0 / (2 * rows * 128)
    scalars = pl.BlockSpec(memory_space=pltpu.SMEM)
    vmem = pl.BlockSpec(memory_space=pltpu.VMEM)
    f32, bf16 = jnp.float32, jnp.bfloat16
    tiles, halves = (3, 32, 128), (3, 16, 128)
    coeffs = pl.pallas_call(
        functools.partial(gather_dot, plan),
        out_shape=jax.ShapeDtypeStruct((rows, 2 * PART), bf16),
        in_specs=[pl.BlockSpec(memory_space=pltpu.HBM)] * 2,
        out_specs=vmem,
        scratch_shapes=[
            pltpu.VMEM((CHUNKS, 4, 4, 2, ROWS, KC), bf16),
            pltpu.VMEM((expansion_basis.shape[1], expansion_basis.shape[0]), bf16),
            pltpu.VMEM(images.shape, bf16),
            pltpu.VMEM((rows, 2 * PART), f32),
            pltpu.SemaphoreType.DMA((2,)),
            pltpu.SemaphoreType.DMA,
            pltpu.SemaphoreType.DMA((len(plan.sems),)),
        ],
        compiler_params=pltpu.CompilerParams(
            collective_id=0, has_side_effects=True, vmem_limit_bytes=52 * 1024 * 1024
        ),
    )(images, pltpu.with_memory_space_constraint(expansion_basis.T, pltpu.HBM))
    packed, begin = pl.pallas_call(
        cut_windows,
        out_shape=(jax.ShapeDtypeStruct((4, 2, *tiles), f32), jax.ShapeDtypeStruct((3, L * KMAX, 128), f32)),
        in_specs=[scalars, scalars, vmem, vmem],
        out_specs=(vmem, vmem),
        scratch_shapes=[pltpu.VMEM((PART, PART), f32)],
        compiler_params=pltpu.CompilerParams(vmem_limit_bytes=16 * 1024 * 1024),
    )(block_sizes, keep_count, coeffs, start_block.swapaxes(1, 2))
    everything = pl.pallas_call(
        functools.partial(reduce_iterate, scale),
        out_shape=jax.ShapeDtypeStruct((L * KMAX, 128), f32),
        in_specs=[vmem, vmem],
        out_specs=vmem,
        scratch_shapes=[
            pltpu.VMEM((4, *tiles), f32),
            pltpu.VMEM((2, 4, *halves), f32),
            pltpu.VMEM((2, 3, *halves), f32),
            pltpu.VMEM((2, 4, *halves), f32),
            pltpu.VMEM((2, 4, *halves), f32),
            pltpu.VMEM((8, 2 * KMAX, 128), f32),
            pltpu.SemaphoreType.DMA((2,)),
            pltpu.SemaphoreType.DMA((3, 2, 2, 3)),
            pltpu.SemaphoreType.DMA((2, 7)),
        ],
        compiler_params=pltpu.CompilerParams(
            collective_id=1, has_side_effects=True, vmem_limit_bytes=16 * 1024 * 1024
        ),
    )(packed, begin)
    features, values = pl.pallas_call(
        project,
        out_shape=(
            jax.ShapeDtypeStruct((rows, 2 * L * KMAX), f32),
            jax.ShapeDtypeStruct((KMAX, L), f32),
        ),
        in_specs=[scalars, vmem, vmem],
        out_specs=(vmem, vmem),
        compiler_params=pltpu.CompilerParams(vmem_limit_bytes=16 * 1024 * 1024),
    )(block_sizes, coeffs, everything)
    return features, values.T


def solution(mesh):
    split = Mesh(mesh.devices.reshape(4, 4, 2, mesh.shape["grp"]), AXES)
    in_specs = (P(AXES, None), P(None, IMG), P(), P(), P())
    out_specs = (P(AXES, None), P())
    return jax.shard_map(
        per_device, mesh=split, in_specs=in_specs, out_specs=out_specs, check_vma=False
    )
```

```python
import functools
import heapq

import jax
import jax.numpy as jnp
from jax import lax
from jax.experimental import pallas as pl
from jax.experimental.pallas import tpu as pltpu
from jax.sharding import Mesh
from jax.sharding import PartitionSpec as P

NMAX = 80
L = 16
S = 480
KMAX = 8
ITERS = 3
AXES = ("img_0", "img_1", "img_2", "grp")
IMG = AXES[:3]
HIGH = lax.Precision.HIGHEST
MESH = pl.DeviceIdType.MESH

KC = 256
SUBS = 4
SIZES = (1, 2, 1, 1, 1)
CHUNKS = 36
ROWS = 32
BLOCK = ROWS * KC * 2
PLANE = (-1, 1, -1, 1)
FIRST_FAR = (2, 1, 3)
PART = 16 * ROWS
WIN = 96


class Plan:
    def __init__(
        self, window=2.5, late=0.3, turns=0.5, spare=-1.0, rate=42.5e3, hop=2.8, d_rate=600e3, d_hop=1.4, dot=0.25, queue=3
    ):
        self.program = []
        self.sems = {}
        self.now = 0.0
        busy, pending, arrived = {}, {}, {}
        heap, ready = [], []
        count = iter(range(10**6))

        def to_go(key):
            r, sub, da, db, dx = key
            forward = -1 if sub % 2 == 0 else 1
            if dx:
                return 1 if dx == forward else 0
            hops = 2 if r == 0 else 0
            if db == 0:
                return hops + 2 + (da == forward)
            return hops + (db == forward)

        def issue(key, link, size):
            sem = self.sems.setdefault(key, len(self.sems))
            end = max(busy.get(link, 0.0), self.now) + size / (d_rate if link == "d" else rate)
            busy[link] = end
            heapq.heappush(heap, (end + (d_hop if link == "d" else hop), sem, key))
            self.program.append(("send", key))

        def pump():
            for link, line in pending.items():
                while line and busy.get(link, 0.0) < self.now + window:
                    _, _, key, size = heapq.heappop(line)
                    issue(key, link, size)

        def enqueue(link, rank, key):
            heapq.heappush(pending.setdefault(link, []), (rank, next(count), key, SIZES[key[0]] * BLOCK))

        def along(axis, place, at, key):
            forward = -1 if key[1] % 2 == 0 else 1
            if place == 0:
                steps = ((-1, "+"), (1, "-"))
            elif place == forward:
                steps = ((2, "+" if forward == -1 else "-"),)
            else:
                steps = ()
            for there, sign in steps:
                onto = key[:at] + (there,) + key[at + 1 :]
                enqueue(axis + sign, onto[0] * late + onto[1] * turns - to_go(onto), onto)

        def onward(key):
            r, sub, da, db, dx = key
            first, second = ("y", "z") if sub < 2 else ("z", "y")
            if dx == 0:
                if db == 0:
                    along(first, da, 2, key)
                along(second, db, 3, key)
            if r == 0 and (da, db) not in ((0, 0), (PLANE[sub], 0)):
                along("x", dx, 4, key)

        def got(group, need):
            arrived[group] = arrived.get(group, 0) + 1
            return arrived[group] == need

        for r in range(len(SIZES)):
            for sub in range(SUBS):
                onward((r, sub, 0, 0, 0))
        for sub in range(SUBS):
            for dx in (-1, 1, 2):
                if PLANE[sub]:
                    link = ("y" if sub < 2 else "z") + ("+" if PLANE[sub] < 0 else "-")
                    enqueue(link, spare + sub * turns, (0, sub, PLANE[sub], 0, dx))
        pump()
        while heap or ready:
            if ready and (not heap or heap[0][0] > self.now or len(ready) > queue):
                self.program.append(("dot", ready.pop(0)))
                self.now += dot
            else:
                when, _, key = heapq.heappop(heap)
                self.now = max(self.now, when) + 0.02
                self.program.append(("wait", key))
                if key[0] == "D":
                    chunk = key[1:4]
                else:
                    onward(key)
                    chunk = (key[0], key[1], key[4])
                    if got((*chunk, "line", key[3]), 4 if key[3] else 3):
                        issue(("D", *chunk, key[3]), "d", 4 * BLOCK * SIZES[key[0]])
                if got(chunk, 19):
                    ready.extend((*chunk, k) for k in range(SIZES[chunk[0]]))
            pump()
        self.end = self.now


def turn(v, by):
    return lax.rem(v + (by + 4), 4)


def device(axis, by):
    spot = dict(zip("yzcx", (lax.axis_index(a) for a in AXES)))
    spot[axis] = turn(spot[axis], by)
    return tuple(spot[a] for a in "yzcx")


def gather_dot(plan, images, basis, coeffs, held, stage, pixels, total, fill_sem, send_sem, recv_sem):
    y, z, c, x = (lax.axis_index(a) for a in AXES)
    sibling = (y, z, 1 - c, x)
    barrier = pltpu.get_barrier_semaphore()
    own = pltpu.make_async_copy(basis, stage, fill_sem.at[0])
    own.start()
    for peer in [device(axis, by) for axis in "yzx" for by in (1, -1)] + [sibling]:
        pl.semaphore_signal(barrier, inc=1, device_id=peer, device_id_type=MESH)
    total[...] = jnp.zeros_like(total)
    own.wait()
    fill = pltpu.make_async_copy(images, pixels, fill_sem.at[1])
    fill.start()
    for k in range(CHUNKS):
        held[k, y, z, c] = jnp.zeros((ROWS, KC), jnp.bfloat16)
        held[k, y, z, c, : stage.shape[0]] = stage[:, k * KC : (k + 1) * KC]
    pl.semaphore_wait(barrier, 7)

    def index(r, sub, dx):
        if r == 0:
            return SUBS * turn(x, dx) + sub
        return SUBS * (4 + sum(SIZES[1:r])) + sub * SIZES[r]

    def copy_of(key):
        if key[0] == "D":
            r, sub, dx, db = key[1:]
            k = pl.ds(index(r, sub, dx), SIZES[r])
            part = held.at[k, :, turn(z, db), c] if sub < 2 else held.at[k, turn(y, db), :, c]
            where = sibling
        else:
            r, sub = key[:2]
            place = list(key[2:])
            moving = 2 if place[2] and place[:2] != [PLANE[sub], 0] else 1 if place[1] else 0
            forward = -1 if sub % 2 == 0 else 1
            there = place[moving]
            step = -there if there != 2 else -forward
            place[moving] = 0 if there != 2 else forward
            da, db, dx = place
            dy, dz = (da, db) if sub < 2 else (db, da)
            part = held.at[pl.ds(index(r, sub, dx), SIZES[r]), turn(y, dy), turn(z, dz), c]
            where = device(("yzx" if sub < 2 else "zyx")[moving], step)
        return pltpu.make_async_remote_copy(
            src_ref=part, dst_ref=part, send_sem=send_sem, recv_sem=recv_sem.at[plan.sems[key]],
            device_id=where, device_id_type=MESH,
        )

    sent = []
    loaded = False
    for op, what in plan.program:
        if op == "send":
            copy = copy_of(what)
            copy.start()
            sent.append(copy)
        elif op == "wait":
            copy_of(what).wait_recv()
        else:
            if not loaded:
                fill.wait()
                loaded = True
            k = index(*what[:3]) + what[3]
            block = held[k].reshape(32 * ROWS, KC)
            rows = pixels[:, pl.ds(pl.multiple_of(k * KC, KC), KC)]
            total[...] += lax.dot_general(
                rows, block, (((1,), (1,)), ((), ())), preferred_element_type=jnp.float32
            )
    if not loaded:
        fill.wait()
    for copy in sent:
        copy.wait_send()
    coeffs[...] = total[...].astype(coeffs.dtype)


def places(sizes):
    offsets, firsts = [], []
    offset = jnp.int32(0)
    for l in range(L):
        offsets.append(offset)
        place = lax.div(offset, 30) * ROWS + lax.rem(offset, 30)
        firsts.append(jnp.minimum(lax.div(place, 8) * 8, PART - WIN))
        offset = offset + sizes[l]
    return offsets, firsts


def cut_windows(sizes, keeps, coeffs, start, packed, begin, gram):
    def part_gram(p):
        some = coeffs[:, p * PART : (p + 1) * PART]
        return lax.dot_general(some, some, (((0,), (0,)), ((), ())), preferred_element_type=jnp.float32)

    gram[...] = part_gram(0) + part_gram(1)

    offsets, firsts = places(sizes)

    def window(l):
        left = jnp.minimum(lax.div(firsts[l], 128), 2) * 128
        rows = gram[pl.ds(pl.multiple_of(firsts[l], 8), WIN), pl.ds(pl.multiple_of(left, 128), 256)]
        return pltpu.roll(rows, lax.rem(256 - (firsts[l] - left), 256), 1)[:, :128]

    lane = lax.broadcasted_iota(jnp.int32, (32, 128), 1)
    for pair in range(L // 2):
        one, two = window(2 * pair), window(2 * pair + 1)
        xo, co = pair // 2, pair % 2
        packed[xo, co, 0] = jnp.where(lane < 96, one[:32], pltpu.roll(one[64:], 32, 1))
        packed[xo, co, 1] = jnp.where(lane < 96, two[:32], pltpu.roll(two[64:], 32, 1))
        packed[xo, co, 2] = jnp.where(lane < 64, pltpu.roll(one[32:64], 96, 1), pltpu.roll(two[32:64], 32, 1))

    row = lax.broadcasted_iota(jnp.int32, (KMAX, 128), 0)
    place = lax.broadcasted_iota(jnp.int32, (NMAX, 128), 1)
    inner = lax.broadcasted_iota(jnp.int32, (NMAX, 128), 0)
    for l in range(L):
        slot = lax.rem(firsts[l] + place, ROWS)
        source = lax.div(firsts[l] + place, ROWS) * 30 + slot - offsets[l]
        source = jnp.where(slot < 30, source, -1)
        hit = ((source == inner) & (inner < sizes[l])).astype(jnp.float32)
        lines = slice(KMAX * l, KMAX * l + KMAX)
        begin[0, lines] = jnp.dot(start[l], hit, precision=HIGH, preferred_element_type=jnp.float32)
        begin[1, lines] = jnp.broadcast_to(jnp.sum(hit, axis=0, keepdims=True), (KMAX, 128))
        keep = jnp.minimum(keeps[l], lax.div(sizes[l] + 1, 2))
        begin[2, lines] = (row < keep).astype(jnp.float32)


def iterate(summed, current, inside, alive):
    wide = lax.broadcasted_iota(jnp.int32, (128, 128), 1)
    block_row = lax.div(lax.broadcasted_iota(jnp.int32, (128, 128), 0), 32) * 32

    def cover_of(i):
        low = jnp.zeros((32, 128), jnp.float32)
        middle = pltpu.roll(summed[2], 32 if i == 0 else 96, 1)
        upper = jnp.concatenate([summed[i], middle, pltpu.roll(summed[i], 96, 1), low], axis=0)
        upper = jnp.where((wide >= block_row) & (wide < WIN), upper, 0.0)
        beyond = jnp.where(wide >= block_row + 32, upper, 0.0)
        return upper + beyond.T

    row = lax.broadcasted_iota(jnp.int32, (KMAX, 128), 0)
    column = lax.broadcasted_iota(jnp.int32, (KMAX, 128), 1)

    def times(current, cover):
        return jnp.dot(current, cover, precision=HIGH, preferred_element_type=jnp.float32)

    covers = [cover_of(i) for i in range(2)]
    lines = [slice(KMAX * i, KMAX * i + KMAX) for i in range(2)]
    currents = [current[i] for i in lines]
    inside = [inside[i] > 0.5 for i in lines]
    alive = [alive[i] > 0.5 for i in lines]
    for turn_id in range(ITERS):
        stacks = [jnp.where(inside[i], times(currents[i], covers[i]), 0.0) for i in range(2)]
        norms = [jnp.ones((KMAX, 1), jnp.float32) for _ in range(2)]
        for m in range(KMAX):
            for i in range(2):
                vector = stacks[i][m : m + 1]
                dots = jnp.sum(stacks[i] * vector, axis=1, keepdims=True)
                square = dots[m : m + 1]
                norms[i] = jnp.where(row[:, :1] == m, square, norms[i])
                if m < KMAX - 1:
                    stacks[i] = jnp.where(row > m, stacks[i] - dots / square * vector, stacks[i])
        currents = [jnp.where(alive[i], stacks[i] / jnp.sqrt(norms[i]), 0.0) for i in range(2)]
    ends = []
    for i in range(2):
        quotient = jnp.sum(currents[i] * times(currents[i], covers[i]), axis=1, keepdims=True)
        ends.append(jnp.where(column == 127, quotient, currents[i]))
    return jnp.concatenate(ends, axis=0)


def reduce_iterate(scale, packed, begin, everything, mate, half, by_x, one, two, found, mate_sem, far_sem, found_sem):
    y, z, c, x = (lax.axis_index(a) for a in AXES)
    sibling = (y, z, 1 - c, x)
    owners = [device("x", by) for by in (1, 2, 3)] + [(y, z, 1 - c, turn(x, by)) for by in range(4)]
    barrier = pltpu.get_barrier_semaphore()
    for peer in owners + [device(axis, by) for axis in "yz" for by in (1, 2, 3)]:
        pl.semaphore_signal(barrier, inc=1, device_id=peer, device_id_type=MESH)
    pl.semaphore_wait(barrier, 13)
    sent = []

    def push(src, dst, sems, where):
        copy = pltpu.make_async_remote_copy(
            src_ref=src, dst_ref=dst, send_sem=sems[0], recv_sem=sems[1], device_id=where, device_id_type=MESH
        )
        copy.start()
        sent.append(copy)
        return copy

    def far(stage, h):
        return [(far_sem.at[stage, h, 0, by - 1], far_sem.at[stage, h, 1, by - 1]) for by in (1, 2, 3)]

    push(packed.at[:, 1 - c], mate, (mate_sem.at[0], mate_sem.at[1]), sibling).wait_recv()
    copies = []
    for h in range(2):
        lines = slice(16 * h, 16 * h + 16)
        for xo in range(4):
            half[h, xo] = packed[xo, c, :, lines] + mate[xo, :, lines]
        copies.append([
            push(half.at[h, turn(x, by)], by_x.at[h, by - 1], far(0, h)[by - 1], device("x", by)) for by in FIRST_FAR
        ])
    for stage, (land, spots, axes) in enumerate(((one, (y, z), "yz"), (two, (z, y), "zy"))):
        onward = []
        for h in range(2):
            for copy in copies[h]:
                copy.wait_recv()
            spot = spots[h]
            if stage == 0:
                land[h, spot] = half[h, x] + by_x[h, 0] + by_x[h, 1] + by_x[h, 2]
            else:
                land[h, spot] = one[h, 0] + one[h, 1] + one[h, 2] + one[h, 3]
            onward.append([
                push(land.at[h, spot], land.at[h, spot], far(1 + stage, h)[by - 1], device(axes[h], by))
                for by in FIRST_FAR
            ])
        copies = onward
    for h in range(2):
        for copy in copies[h]:
            copy.wait_recv()
    sums = [two[h, 0] + two[h, 1] + two[h, 2] + two[h, 3] for h in range(2)]
    summed = jnp.concatenate(sums, axis=1) * scale

    me = 2 * x + c
    lines = pl.ds(pl.multiple_of(2 * KMAX * me, 2 * KMAX), 2 * KMAX)
    found[me] = iterate(summed, begin[0, lines], begin[1, lines], begin[2, lines])
    copies = [push(found.at[me], found.at[me], (found_sem.at[0, e], found_sem.at[1, e]), owners[e]) for e in (1, 5, 0, 2, 4, 6, 3)]
    for copy in copies:
        copy.wait_recv()
    everything[...] = found[...].reshape(L * KMAX, 128)
    for copy in sent:
        copy.wait_send()


def project(sizes, coeffs, everything, features, values):
    firsts = places(sizes)[1]
    tall = lax.broadcasted_iota(jnp.int32, (L * KMAX, 128), 0)
    wide = lax.broadcasted_iota(jnp.int32, (L * KMAX, 128), 1)
    spread = jnp.where(lax.div(tall, KMAX) == wide, everything[:, 127:128], 0.0)
    choose = lax.rem(wide[:KMAX], KMAX) == tall[:KMAX]
    values[...] = jnp.dot(
        choose.astype(jnp.float32), spread, precision=HIGH, preferred_element_type=jnp.float32
    )[:, :L]
    lines = []
    for l in range(L):
        line = jnp.where(wide[:KMAX] < WIN, everything[KMAX * l : KMAX * l + KMAX], 0.0)
        line = jnp.concatenate([line, jnp.zeros((KMAX, PART - 128), jnp.float32)], axis=1)
        lines.append(pltpu.roll(line, firsts[l], 1))
    rounded = jnp.concatenate(lines, axis=0).astype(jnp.bfloat16)
    for p in range(2):
        features[:, p * 128 : (p + 1) * 128] = lax.dot_general(
            coeffs[:, p * PART : (p + 1) * PART], rounded, (((1,), (1,)), ((), ())),
            preferred_element_type=jnp.float32,
        )


def per_device(images, expansion_basis, block_sizes, keep_count, start_block):
    plan = Plan()
    rows = images.shape[0]
    scale = 1.0 / (2 * rows * 128)
    scalars = pl.BlockSpec(memory_space=pltpu.SMEM)
    vmem = pl.BlockSpec(memory_space=pltpu.VMEM)
    f32, bf16 = jnp.float32, jnp.bfloat16
    tiles, halves = (3, 32, 128), (3, 16, 128)
    coeffs = pl.pallas_call(
        functools.partial(gather_dot, plan),
        out_shape=jax.ShapeDtypeStruct((rows, 2 * PART), bf16),
        in_specs=[pl.BlockSpec(memory_space=pltpu.HBM)] * 2,
        out_specs=vmem,
        scratch_shapes=[
            pltpu.VMEM((CHUNKS, 4, 4, 2, ROWS, KC), bf16),
            pltpu.VMEM((expansion_basis.shape[1], expansion_basis.shape[0]), bf16),
            pltpu.VMEM(images.shape, bf16),
            pltpu.VMEM((rows, 2 * PART), f32),
            pltpu.SemaphoreType.DMA((2,)),
            pltpu.SemaphoreType.DMA,
            pltpu.SemaphoreType.DMA((len(plan.sems),)),
        ],
        compiler_params=pltpu.CompilerParams(
            collective_id=0, has_side_effects=True, vmem_limit_bytes=52 * 1024 * 1024
        ),
    )(images, pltpu.with_memory_space_constraint(expansion_basis.T, pltpu.HBM))
    packed, begin = pl.pallas_call(
        cut_windows,
        out_shape=(jax.ShapeDtypeStruct((4, 2, *tiles), f32), jax.ShapeDtypeStruct((3, L * KMAX, 128), f32)),
        in_specs=[scalars, scalars, vmem, vmem],
        out_specs=(vmem, vmem),
        scratch_shapes=[pltpu.VMEM((PART, PART), f32)],
        compiler_params=pltpu.CompilerParams(vmem_limit_bytes=16 * 1024 * 1024),
    )(block_sizes, keep_count, coeffs, start_block.swapaxes(1, 2))
    everything = pl.pallas_call(
        functools.partial(reduce_iterate, scale),
        out_shape=jax.ShapeDtypeStruct((L * KMAX, 128), f32),
        in_specs=[vmem, vmem],
        out_specs=vmem,
        scratch_shapes=[
            pltpu.VMEM((4, *tiles), f32),
            pltpu.VMEM((2, 4, *halves), f32),
            pltpu.VMEM((2, 3, *halves), f32),
            pltpu.VMEM((2, 4, *halves), f32),
            pltpu.VMEM((2, 4, *halves), f32),
            pltpu.VMEM((8, 2 * KMAX, 128), f32),
            pltpu.SemaphoreType.DMA((2,)),
            pltpu.SemaphoreType.DMA((3, 2, 2, 3)),
            pltpu.SemaphoreType.DMA((2, 7)),
        ],
        compiler_params=pltpu.CompilerParams(
            collective_id=1, has_side_effects=True, vmem_limit_bytes=16 * 1024 * 1024
        ),
    )(packed, begin)
    features, values = pl.pallas_call(
        project,
        out_shape=(
            jax.ShapeDtypeStruct((rows, 2 * L * KMAX), f32),
            jax.ShapeDtypeStruct((KMAX, L), f32),
        ),
        in_specs=[scalars, vmem, vmem],
        out_specs=(vmem, vmem),
        compiler_params=pltpu.CompilerParams(vmem_limit_bytes=16 * 1024 * 1024),
    )(block_sizes, coeffs, everything)
    return features, values.T


def solution(mesh):
    split = Mesh(mesh.devices.reshape(4, 4, 2, mesh.shape["grp"]), AXES)
    in_specs = (P(AXES, None), P(None, IMG), P(), P(), P())
    out_specs = (P(AXES, None), P())
    return jax.shard_map(
        per_device, mesh=split, in_specs=in_specs, out_specs=out_specs, check_vma=False
    )
```
